32 devices in a mesh: mp: 2 (over core), tile: 16 (over z, y, x).
Axes of the slice: x: 2, y: 2, z: 4, core: 2. Of those that a mesh axis runs over, the one named last changes fastest.
Arguments:
- state: float32 [2, 20, 64, 1024], P('mp', None, 'tile'), may hold values from -6 to 6
- guess: float32 [2, 24, 64, 1024], P('mp', None, 'tile'), may hold values from -6 to 6
- regrid: bfloat16 [2, 16, 16, 256, 256], P('mp', 'tile'), may hold values from -1 to 1
- regime: int32 [2, 64, 1024], P('mp', 'tile'), may hold values from 0 to 3
- land: int32 [2, 64, 1024], P('mp', 'tile'), may hold values 0 or 1
- land_temp: float32 [2, 64, 1024], P('mp', 'tile'), may hold values from -6 to 6
- exchange_rate: float32 [2, 4], P('mp'), may hold values from 0.05 to 0.3
- vertical: float32 [2, 19], P('mp'), may hold values from 0.05 to 0.3
- mixing: float32 [2], P('mp'), may hold values from 0.02 to 0.1
Outputs:
- final_state: float32 [2, 20, 64, 1024], P('mp', None, 'tile')
- forcing: float32 [2, 24, 64, 1024], P('mp', None, 'tile')
The draws below stay inside these ranges and needn't reach their ends.
All inputs are finite; a program needn't handle non-finite values. No bound on the sum of `land` on one device may be relied on, other than what follows from the above.
Results may differ from the reference program's by a relative error of at most 0.0029.
Values may be sent and summed in bfloat16 or wider, within the bound.
No kernel may reach another device: no remote copies, remote signals or barrier semaphores. Data moves between devices by JAX's collectives and lax.ppermute only.
A program may use at most 128 MiB of HBM per device.

```python
import math
import jax
import jax.numpy as jnp
from jax import lax

LEV = 20
NT = 24
ITERS = 2
REGIMES = 4
FACE = 64
ROWS = 4
TILES = 16
COLS = 1024
GRID_ROWS = 64
SUB = 256


def draw_regrid(key, part):
    base = jax.random.fold_in(key, 7)
    first_key, second_key = jax.random.split(base)
    shape = (2, TILES, TILES, SUB, SUB)
    identity = jnp.eye(SUB, dtype=jnp.float32)
    spread = jax.random.normal(first_key, shape, jnp.float32) * (0.5 / math.sqrt(SUB))
    diagonal = jax.random.uniform(second_key, shape[:-1], jnp.float32, 0.45, 0.55)
    blocks = spread + diagonal[..., None] * identity
    return jnp.clip(blocks, -1.0, 1.0).astype(jnp.bfloat16)


def with_ends(values, stream_key, least, high):
    longest = values.shape.index(max(values.shape))
    spots = []
    for shift in (0, 1):
        where = [jax.random.randint(jax.random.fold_in(stream_key, axis), (), 0, length) for axis, length in enumerate(values.shape)]
        where[longest] = (where[longest] + shift) % values.shape[longest]
        spots.append(tuple(where))
    return values.at[spots[0]].set(least).at[spots[1]].set(high)


def block_scale(key, extent, cuts, low, largest):
    gain, own = 1.0, jax.random.fold_in(key, 6)
    for dim, blocks in cuts:
        draws = jnp.exp(jax.random.uniform(jax.random.fold_in(own, dim), (blocks,), jnp.float32, low / len(cuts), largest / len(cuts)))
        gain = gain * jnp.repeat(draws, extent[dim] // blocks).reshape([-1 if axis == dim else 1 for axis in range(len(extent))])
    return gain


def centred(own_key, dims, scale, limit, cuts=(), kind=jnp.bfloat16):
    drawn = jax.random.normal(own_key, dims, jnp.float32) * scale
    if len(cuts) > 0:
        drawn = block_scale(own_key, dims, cuts, -0.22, 0.18) * drawn
    return jnp.clip(drawn, min=-limit, max=limit).astype(kind)


def setup_inputs(seed: int = 0) -> dict:
    keys = jax.random.split(jax.random.key(seed), 10)
    state = centred(keys[0], (2, LEV, GRID_ROWS, COLS), 1.0, 6.0, ((0, 2), (2, 16)), jnp.float32)
    guess = centred(keys[1], (2, NT, GRID_ROWS, COLS), 1.0, 6.0, ((0, 2), (2, 16)), jnp.float32)
    regrid = draw_regrid(jax.random.fold_in(keys[9], 71), 0)
    regime = with_ends(jax.random.randint(keys[3], (2, GRID_ROWS, COLS), 0, REGIMES), jax.random.fold_in(keys[3], 1), 0, REGIMES - 1).astype(jnp.int32)
    land = with_ends((jax.random.randint(keys[4], (2, GRID_ROWS, COLS), 0, 10) < 3).astype(jnp.int32), jax.random.fold_in(keys[4], 1), 0, 1)
    land_temp = centred(keys[5], (2, GRID_ROWS, COLS), 1.0, 6.0, ((0, 2), (1, 16)), jnp.float32)
    exchange_rate = jnp.clip(jnp.exp(math.log(0.3) - 1.7917595 * jax.random.uniform(keys[6], (2, REGIMES), jnp.float32) ** block_scale(keys[6], (2, REGIMES), ((0, 2),), -0.2, 0.2)), 0.05, 0.3)
    vertical = jnp.clip(jnp.exp(math.log(0.3) - 1.7917595 * jax.random.uniform(keys[7], (2, LEV - 1), jnp.float32) ** block_scale(keys[7], (2, LEV - 1), ((0, 2),), -0.2, 0.2)), 0.05, 0.3)
    mixing = jnp.clip(jnp.exp(math.log(0.1) - 1.609438 * jax.random.uniform(keys[8], (2,), jnp.float32) ** block_scale(keys[8], (2,), ((0, 2),), -0.2, 0.2)), 0.02, 0.1)
    return dict(state=state, guess=guess, regrid=regrid, regime=regime, land=land, land_temp=land_temp, exchange_rate=exchange_rate, vertical=vertical, mixing=mixing)


def rate_field(regime, rates):
    field = jnp.zeros(regime.shape, jnp.float32)
    for kind_index in range(REGIMES):
        field = field + jnp.where(regime == kind_index, rates[kind_index], jnp.zeros((), jnp.float32))
    return field


def advance(column, force_now, coeff, land, land_temp, vertical, mixing):
    surface = column[0]
    boundary = jnp.where(land == 1, land_temp, force_now)
    flux = coeff * (boundary - surface)
    padded = jnp.pad(surface, ((1, 1), (0, 0)))
    lateral = padded[2:] + padded[:-2] + jnp.roll(surface, 1, axis=1) + jnp.roll(surface, -1, axis=1) - 4.0 * surface
    between = vertical[:, None, None] * (column[1:] - column[:-1])
    change = jnp.pad(between, ((0, 1), (0, 0), (0, 0))) - jnp.pad(between, ((1, 0), (0, 0), (0, 0)))
    updated = column + change
    updated = updated.at[0].add(flux + mixing * lateral)
    return updated


def run_window(column, forcing, coeff, land, land_temp, vertical, mixing):
    def one_step(carry, force_now):
        updated = advance(carry, force_now, coeff, land, land_temp, vertical, mixing)
        return updated, updated[0].astype(jnp.bfloat16)
    return lax.scan(one_step, column, forcing)


def regrid_trace(blocks, trace):
    pieces = trace.reshape(NT, TILES, ROWS, TILES, FACE).astype(jnp.float32)
    shaped = blocks.reshape(TILES, TILES, ROWS, FACE, ROWS, FACE).astype(jnp.float32)
    result = jnp.einsum('tarow,oapqrw->topaq', pieces, shaped, precision=lax.Precision.HIGHEST)
    return result.reshape(NT, GRID_ROWS, COLS)


def reference(state, guess, regrid, regime, land, land_temp, exchange_rate, vertical, mixing):
    coeffs = [rate_field(regime[member], exchange_rate[member]) for member in range(2)]
    forcing = guess
    finals = []
    for sweep_index in range(ITERS):
        finals = []
        traces = []
        for member in range(2):
            column, trace = run_window(state[member], forcing[member], coeffs[member], land[member], land_temp[member], vertical[member], mixing[member])
            finals.append(column)
            traces.append(trace)
        forcing = jnp.stack([regrid_trace(regrid[0], traces[1]), regrid_trace(regrid[1], traces[0])])
    return jnp.stack(finals), forcing
```

```python
import functools

import jax
import jax.numpy as jnp
from jax import lax
from jax.experimental import pallas as pl
from jax.experimental.pallas import tpu as pltpu
from jax.sharding import PartitionSpec as P

ITERS = 2
LANES = 128
SUBLANES = 8
EXACT = lax.Precision.HIGHEST
SMEM = pl.BlockSpec(memory_space=pltpu.SMEM)
VMEM = pl.BlockSpec(memory_space=pltpu.VMEM)


def lane_of(shape):
    return lax.broadcasted_iota(jnp.int32, shape, len(shape) - 1)


def row_of(shape):
    return lax.broadcasted_iota(jnp.int32, shape, 0)


def tiles_of(width):
    return [pl.ds(k * LANES, LANES) for k in range(width // LANES)]


def windows(tile, count, face):
    half = (LANES - face) // 2
    for k in range(count):
        own, left, right = tile(k), tile((k - 1) % count), tile((k + 1) % count)
        lane = lane_of(own.shape)
        yield 2 * k, jnp.where(lane < face + half, own, left)
        yield 2 * k + 1, pltpu.roll(jnp.where(lane < half, right, own), face, axis=1)


def joined(first, second, face):
    out = []
    for j in range(first.shape[1] // LANES):
        cut = slice(j * LANES, (j + 1) * LANES)
        x, y = first[:, cut], second[:, cut]
        lane = lane_of(x.shape)
        out.append(jnp.where(lane < face, x, pltpu.roll(y, face, axis=1)))
        out.append(jnp.where(lane < face, pltpu.roll(x, face, axis=1), y))
    return out


def prepare(rates, vertical, state, guess, regime, land, land_temp, chunk, base, sea, mats, memory, xs, by_row, levels):
    lev, rows, width = state.shape
    steps = guess.shape[0]
    padded = xs.shape[0] // (steps + 1)
    face = width // chunk.shape[0]

    shape = (padded, LANES)
    row, lane = row_of(shape), lane_of(shape)
    up = jnp.zeros(shape, jnp.float32)
    down = jnp.zeros(shape, jnp.float32)
    for l in range(lev - 1):
        up = jnp.where((row == l) & (row > 0), vertical[0, l], up)
        down = jnp.where(row == l + 1, vertical[0, l], down)
    keep = jnp.where(row == 0, 0.0, 1.0 - up - down)
    power = jnp.where((row == lane) & (row < lev), 1.0, 0.0)
    answer = jnp.zeros(shape, jnp.float32)
    for n in range(steps + 1):
        xs[pl.ds(n * padded, padded), :] = power
        if n == steps:
            break
        answer = jnp.where(lane == steps - 1 - n, power[:, 0:1], answer)
        power = keep * power + up * pltpu.roll(power, padded - 1, axis=0) + down * pltpu.roll(power, 1, axis=0)
    mats[0] = jnp.where(row == 0, 0.0, power)
    mats[1] = answer
    first = xs[pl.ds(1, steps, stride=padded), :]
    v0 = vertical[0, 0]
    memory[...] = jnp.broadcast_to(v0 * first[:, 0:1], first.shape)
    to_below = jnp.where(lane_of(first.shape) == 0, 0.0, v0 * first)[:, :padded]

    coeff = jnp.zeros(regime.shape, jnp.float32)
    for kind in range(rates.shape[1]):
        coeff = jnp.where(regime[...] == kind, rates[0, kind], coeff)
    on_land = land[...] == 1
    sea[...] = jnp.where(on_land, 0.0, coeff)
    fixed = jnp.where(on_land, coeff * land_temp[...], 0.0)

    count = width // LANES
    rest = pl.ds(lev * rows, (padded - lev) * rows)
    for k, cut in enumerate(tiles_of(width)):
        for l in range(lev):
            levels[k, pl.ds(l * rows, rows), :] = state[l, :, cut]
        levels[k, rest, :] = jnp.zeros((rest.size, LANES), jnp.float32)
        for t in range(steps):
            by_row[k, pl.ds(t * rows, rows), :] = guess[t, :, cut]
    for p in range(rows):
        drives = []
        for k, cut in enumerate(tiles_of(width)):
            own = levels[k, pl.ds(p, padded, stride=rows), :]
            below = jnp.dot(to_below, own, precision=EXACT, preferred_element_type=jnp.float32)
            part = below + fixed[p : p + 1, k * LANES : (k + 1) * LANES]
            base[p, :, cut] = part
            drives.append(part + sea[p : p + 1, cut] * by_row[k, pl.ds(p, steps, stride=rows), :])
        for a, window in windows(lambda k: drives[k], count, face):
            chunk[a, pl.ds(p * steps, steps), :] = window.astype(jnp.bfloat16)
    fields = jnp.concatenate([state[0], regime[...].astype(jnp.float32)], axis=0)
    for a, window in windows(lambda k: fields[:, k * LANES : (k + 1) * LANES], count, face):
        chunk[a, pl.ds(rows * steps, 2 * rows), :] = window.astype(jnp.bfloat16)


def evolve(first, rates, vertical, mixing, memory, arrived, *refs):
    if first:
        fields, trace, drive, past, packed = refs
    else:
        fields, trace, drive, past, packed = refs
    tiles, steps, cells = trace.shape
    grid_rows = fields.shape[1]
    rows = grid_rows // tiles
    face = cells // rows
    held = rows * steps
    for a in range(tiles):
        drive[pl.ds(a * held, held), :] = arrived[a, pl.ds(0, held), :].astype(jnp.float32)
    side = pl.ds(SUBLANES, grid_rows)
    if first:
        for a in range(tiles):
            both = arrived[a, pl.ds(held, 2 * rows), :].astype(jnp.float32)
            fields[0, pl.ds(a * rows, rows), :] = both[:rows]
            fields[1, pl.ds(a * rows, rows), :] = both[rows:]
        regime = fields[1]
        coeff = jnp.zeros(regime.shape, jnp.float32)
        for kind in range(rates.shape[1]):
            coeff = jnp.where(regime == kind, rates[0, kind], coeff)
        fields[1] = 1.0 - vertical[0, 0] - coeff - 4.0 * mixing[0]
    stay = fields[1]
    mix = mixing[0]
    edge = jnp.zeros((SUBLANES, LANES), jnp.float32)
    for n in range(steps + 1):
        past[n, pl.ds(0, SUBLANES), :] = edge
        past[n, pl.ds(SUBLANES + grid_rows, SUBLANES), :] = edge
    surface = fields[0]
    past[0, side, :] = surface
    lane = lane_of((tiles, LANES))
    for n in range(steps):
        known = drive[pl.ds(n, grid_rows, stride=steps), :]
        for k in range(n):
            known = known + memory[n - k : n - k + 1, :] * past[k, side, :]
        lateral = past[n, pl.ds(SUBLANES - 1, grid_rows), :] + past[n, pl.ds(SUBLANES + 1, grid_rows), :]
        lateral = lateral + (pltpu.roll(surface, 1, axis=1) + pltpu.roll(surface, LANES - 1, axis=1))
        surface = (stay * surface + known) + mix * lateral
        past[n + 1, side, :] = surface
        for j in range(cells // LANES):
            even = past[n + 1, pl.ds(SUBLANES + 2 * j, tiles, stride=rows), :]
            odd = past[n + 1, pl.ds(SUBLANES + 2 * j + 1, tiles, stride=rows), :]
            packed[j, pl.ds(n, tiles, stride=steps), :] = jnp.where(lane < face, even, pltpu.roll(odd, face, axis=1))
    for j in range(cells // LANES):
        for a in range(tiles):
            trace[a, :, pl.ds(j * LANES, LANES)] = packed[j, pl.ds(a * steps, steps), :].astype(jnp.bfloat16)


def product(trace, regrid, a):
    return lax.dot_general(trace[a], regrid[a], (((1,), (1,)), ((), ())), preferred_element_type=jnp.float32)


def redrive(trace, regrid, base, sea, chunk, drive):
    tiles, steps, cells = trace.shape
    rows, _, width = base.shape
    face = cells // rows
    count = width // LANES
    for k, cut in enumerate(tiles_of(width)):
        mapped = joined(product(trace, regrid, 2 * k), product(trace, regrid, 2 * k + 1), face)
        for p in range(rows):
            drive[p, :, cut] = base[p, :, cut] + sea[p : p + 1, cut] * mapped[p]
    for p in range(rows):
        for a, window in windows(lambda k: drive[p, :, k * LANES : (k + 1) * LANES], count, face):
            chunk[a, pl.ds(p * steps, steps), :] = window.astype(jnp.bfloat16)


def remap(trace, regrid, forcing, by_row):
    tiles, steps, cells = trace.shape
    _, rows, width = forcing.shape
    face = cells // rows
    for k, cut in enumerate(tiles_of(width)):
        mapped = joined(product(trace, regrid, 2 * k), product(trace, regrid, 2 * k + 1), face)
        for p in range(rows):
            by_row[k, pl.ds(p, steps, stride=rows), :] = mapped[p]
        for t in range(steps):
            forcing[t, :, cut] = by_row[k, pl.ds(t * rows, rows), :]


def finish(history, state, mats, final, levels, by_row):
    tiles, steps, cells = history.shape
    lev, rows, width = state.shape
    padded = levels.shape[1] // rows
    face = cells // rows
    rest = pl.ds(lev * rows, (padded - lev) * rows)
    still = mats[0][:, :padded]
    answer = mats[1][:, :steps]
    for k, cut in enumerate(tiles_of(width)):
        for l in range(lev):
            levels[k, pl.ds(l * rows, rows), :] = state[l, :, cut]
        levels[k, rest, :] = jnp.zeros((rest.size, LANES), jnp.float32)
        seen = joined(history[2 * k].astype(jnp.float32), history[2 * k + 1].astype(jnp.float32), face)
        for p in range(rows):
            own = levels[k, pl.ds(p, padded, stride=rows), :]
            end = jnp.dot(still, own, precision=EXACT, preferred_element_type=jnp.float32)
            end = end + jnp.dot(answer, seen[p], precision=EXACT, preferred_element_type=jnp.float32)
            by_row[k, pl.ds(p, padded, stride=rows), :] = end
        for l in range(lev):
            final[l, :, cut] = by_row[k, pl.ds(l * rows, rows), :]


def on_device(state, guess, regrid, regime, land, land_temp, exchange_rate, vertical, mixing):
    _, lev, rows, width = state.shape
    steps = guess.shape[1]
    tiles = lax.axis_size("tile")
    face = width // tiles
    cells = rows * face
    grid_rows = rows * tiles
    if 2 * face != LANES or LANES - face < 2 * steps or (2 * rows) % SUBLANES or steps % SUBLANES:
        raise ValueError("unsupported sizes")
    padded = -(-lev // SUBLANES) * SUBLANES
    f32, bf16 = jnp.float32, jnp.bfloat16
    shape = jax.ShapeDtypeStruct
    state, guess, blocks = state[0], guess[0], regrid[0, 0]

    chunk, base, sea, mats, memory = pl.pallas_call(
        prepare,
        out_shape=(
            shape((tiles, rows * steps + 2 * rows, LANES), bf16),
            shape((rows, steps, width), f32),
            shape((rows, width), f32),
            shape((2, padded, LANES), f32),
            shape((steps, LANES), f32),
        ),
        in_specs=[SMEM, SMEM] + [VMEM] * 5,
        out_specs=(VMEM,) * 5,
        scratch_shapes=[
            pltpu.VMEM(((steps + 1) * padded, LANES), f32),
            pltpu.VMEM((width // LANES, steps * rows, LANES), f32),
            pltpu.VMEM((width // LANES, padded * rows, LANES), f32),
        ],
        name="prepare",
    )(exchange_rate, vertical, state, guess, regime[0], land[0], land_temp[0])

    fields = None
    for sweep in range(ITERS):
        arrived = lax.all_to_all(chunk, "tile", split_axis=0, concat_axis=0, tiled=True)
        trace_shape = shape((tiles, steps, cells), bf16)
        fields_shape = shape((2, grid_rows, LANES), f32)
        first = fields is None
        got = pl.pallas_call(
            functools.partial(evolve, first),
            out_shape=(fields_shape, trace_shape) if first else trace_shape,
            in_specs=[SMEM] * 3 + [VMEM] * (2 if first else 3),
            out_specs=(VMEM, VMEM) if first else VMEM,
            scratch_shapes=[
                pltpu.VMEM((tiles * rows * steps, LANES), f32),
                pltpu.VMEM((steps + 1, grid_rows + 2 * SUBLANES, LANES), f32),
                pltpu.VMEM((cells // LANES, tiles * steps, LANES), f32),
            ],
            name="evolve",
        )(exchange_rate, vertical, mixing, memory, arrived, *(() if first else (fields,)))
        fields, trace = got if first else (fields, got)
        partner = lax.ppermute(trace, "mp", [(0, 1), (1, 0)])
        if sweep < ITERS - 1:
            chunk = pl.pallas_call(
                redrive,
                out_shape=shape((tiles, rows * steps, LANES), bf16),
                in_specs=[VMEM] * 4,
                out_specs=VMEM,
                scratch_shapes=[pltpu.VMEM((rows, steps, width), f32)],
                name="redrive",
            )(partner, blocks, base, sea)
    forcing = pl.pallas_call(
        remap,
        out_shape=shape((steps, rows, width), f32),
        in_specs=[VMEM] * 2,
        out_specs=VMEM,
        scratch_shapes=[pltpu.VMEM((width // LANES, steps * rows, LANES), f32)],
        name="remap",
    )(partner, blocks)
    history = lax.all_to_all(trace, "tile", split_axis=0, concat_axis=0, tiled=True)
    final = pl.pallas_call(
        finish,
        out_shape=shape((lev, rows, width), f32),
        in_specs=[VMEM] * 3,
        out_specs=VMEM,
        scratch_shapes=[pltpu.VMEM((width // LANES, padded * rows, LANES), f32)] * 2,
        name="finish",
    )(history, state, mats)
    return final[None], forcing[None]


def solution(mesh):
    return jax.shard_map(
        on_device,
        mesh=mesh,
        in_specs=(
            P("mp", None, "tile", None),
            P("mp", None, "tile", None),
            P("mp", "tile", None, None, None),
            P("mp", "tile", None),
            P("mp", "tile", None),
            P("mp", "tile", None),
            P("mp", None),
            P("mp", None),
            P("mp"),
        ),
        out_specs=(P("mp", None, "tile", None), P("mp", None, "tile", None)),
        check_vma=False,
    )
```

```python
import functools
import math

import jax
import jax.numpy as jnp
from jax import lax
from jax.experimental import pallas as pl
from jax.experimental.pallas import tpu as pltpu
from jax.sharding import PartitionSpec as P

ITERS = 2
LANES = 128
SUBLANES = 8
SPARE = 4 << 20
EXACT = lax.Precision.HIGHEST
VMEM = pl.BlockSpec(memory_space=pltpu.VMEM)
HBM = pl.BlockSpec(memory_space=pltpu.HBM)


def size_of(leaf):
    rows = -(-leaf.shape[-2] // SUBLANES) * SUBLANES if len(leaf.shape) > 1 else SUBLANES
    lanes = -(-leaf.shape[-1] // LANES) * LANES
    return math.prod(leaf.shape[:-2]) * rows * lanes * 4


def run(kernel, out, arrays, scratch, far=0, outward=0, cost=1):
    leaves = jax.tree.leaves(out) + list(arrays[far:]) + [leaf for leaf in scratch if hasattr(leaf, "shape")]
    return pl.pallas_call(
        kernel,
        out_shape=out,
        in_specs=[HBM] * far + [VMEM] * (len(arrays) - far),
        out_specs=(VMEM,) * (len(out) - outward) + (HBM,) * outward if isinstance(out, tuple) else VMEM,
        scratch_shapes=[leaf if not isinstance(leaf, jax.ShapeDtypeStruct) else pltpu.VMEM(leaf.shape, leaf.dtype) for leaf in scratch],
        compiler_params=pltpu.CompilerParams(vmem_limit_bytes=sum(map(size_of, leaves)) + SPARE),
        cost_estimate=pl.CostEstimate(flops=cost * 1000000, bytes_accessed=0, transcendentals=0),
        name=getattr(kernel, "__name__", "evolve"),
    )(*[a if a.size == 1 else pltpu.with_memory_space_constraint(a, pltpu.HBM) for a in arrays[:far]], *arrays[far:])


def lane_of(shape):
    return lax.broadcasted_iota(jnp.int32, shape, len(shape) - 1)


def row_of(shape):
    return lax.broadcasted_iota(jnp.int32, shape, 0)


def tiles_of(width):
    return [pl.ds(k * LANES, LANES) for k in range(width // LANES)]


def windows(tile, count, face):
    half = (LANES - face) // 2
    for k in range(count):
        own, left, right = tile(k), tile((k - 1) % count), tile((k + 1) % count)
        lane = lane_of(own.shape)
        yield 2 * k, jnp.where(lane < face + half, own, left)
        yield 2 * k + 1, pltpu.roll(jnp.where(lane < half, right, own), face, axis=1)


def pick(lane, cuts, parts):
    out = parts[-1]
    for cut, part in zip(reversed(cuts), reversed(parts[:-1])):
        out = jnp.where(lane < cut, part, out)
    return out


def ship(drive, chunk, face):
    rows, steps, width = drive.shape
    lane = lane_of((SUBLANES, LANES))
    views = [windows(lambda k, p=p: drive[p, :, k * LANES : (k + 1) * LANES], width // LANES, face) for p in range(rows)]
    for group in zip(*views):
        early, middle, late = [[view[g * SUBLANES : (g + 1) * SUBLANES] for _, view in group] for g in range(3)]
        tiles = []
        for p in range(rows):
            near, far = pltpu.roll(late[p], 24, axis=1), pltpu.roll(late[p], LANES - 24, axis=1)
            tiles.append(pick(lane, (88, 96, 104), (early[p], near, far, early[p])))
        for p in range(0, rows, 2):
            near, far = pltpu.roll(middle[p + 1], 16, axis=1), pltpu.roll(middle[p + 1], LANES - 16, axis=1)
            tiles.append(pick(lane, (80, 96, 112), (middle[p], near, far, middle[p])))
        rest = middle[1::2] + late
        for first, second in zip(rest[::2], rest[1::2]):
            tiles.append(pick(lane, (face,), (first, pltpu.roll(second, face, axis=1))))
        for i, tile in enumerate(tiles):
            chunk[group[0][0], pl.ds(i * SUBLANES, SUBLANES), :] = tile.astype(jnp.bfloat16)


def landed(arrived, a, rows, face, g):
    lane = lane_of((SUBLANES, LANES))
    tile = lambda i: arrived[a, pl.ds(i * SUBLANES, SUBLANES), :].astype(jnp.float32)
    if g == 0:
        return [tile(p) for p in range(rows)]

    def rest(i):
        held = tile(rows + rows // 2 + i // 2)
        return pltpu.roll(held, face, axis=1) if i % 2 else held

    if g == 1:
        out = []
        for p in range(0, rows, 2):
            both = tile(rows + p // 2)
            near, far = pltpu.roll(both, LANES - 16, axis=1), pltpu.roll(both, 16, axis=1)
            out += [both, pick(lane, (face, 96), (rest(p // 2), near, far))]
        return out
    out = []
    for p in range(rows):
        both = tile(p)
        near, far = pltpu.roll(both, LANES - 24, axis=1), pltpu.roll(both, 24, axis=1)
        out.append(pick(lane, (face, 96), (rest(rows // 2 + p), near, far)))
    return out


def joined(first, second, face):
    out = []
    for j in range(first.shape[1] // LANES):
        cut = slice(j * LANES, (j + 1) * LANES)
        x, y = first[:, cut], second[:, cut]
        lane = lane_of(x.shape)
        out.append(jnp.where(lane < face, x, pltpu.roll(y, face, axis=1)))
        out.append(jnp.where(lane < face, pltpu.roll(x, face, axis=1), y))
    return out


def prepare(
    rates_far, vertical_far, mixing_far, regime_far, land_far, land_temp_far, state_far, guess_far, blocks_far,
    chunk, base, sea, mats, memory, blocks,
    xs, by_row, levels, drive, rates, vertical, mixing, regime, land, land_temp, state, guess, done,
):
    pairs = (
        (rates_far, rates),
        (vertical_far, vertical),
        (mixing_far, mixing),
        (regime_far, regime),
        (land_far, land),
        (land_temp_far, land_temp),
        (state_far, state),
        (guess_far, guess),
        (blocks_far, blocks),
    )
    copies = [pltpu.make_async_copy(far, near, done.at[i]) for i, (far, near) in enumerate(pairs)]
    for copy in copies:
        copy.start()
    for copy in copies[:3]:
        copy.wait()
    lev, rows, width = state.shape
    steps = guess.shape[0]
    padded = xs.shape[0] // (steps + 1)
    face = width // chunk.shape[0]

    shape = (padded, LANES)
    row, lane = row_of(shape), lane_of(shape)
    up = jnp.zeros(shape, jnp.float32)
    down = jnp.zeros(shape, jnp.float32)
    for l in range(lev - 1):
        up = jnp.where((row == l) & (row > 0), vertical[0, l], up)
        down = jnp.where(row == l + 1, vertical[0, l], down)
    keep = jnp.where(row == 0, 0.0, 1.0 - up - down)
    power = jnp.where((row == lane) & (row < lev), 1.0, 0.0)
    answer = jnp.zeros(shape, jnp.float32)
    for n in range(steps + 1):
        xs[pl.ds(n * padded, padded), :] = power
        if n == steps:
            break
        answer = jnp.where(lane == steps - 1 - n, power[:, 0:1], answer)
        power = keep * power + up * pltpu.roll(power, padded - 1, axis=0) + down * pltpu.roll(power, 1, axis=0)
    mats[0] = jnp.where(row == 0, 0.0, power)
    mats[1] = answer
    first = xs[pl.ds(1, steps, stride=padded), :]
    v0 = vertical[0, 0]
    memory[pl.ds(0, steps), :] = jnp.broadcast_to(v0 * first[:, 0:1], first.shape)
    shape = (SUBLANES, LANES)
    row = row_of(shape)
    known = jnp.where(row == 0, 1.0 - v0 - 4.0 * mixing[0, 0], mixing[0, 0])
    for kind in range(rates.shape[1]):
        known = jnp.where(row == 2 + kind, rates[0, kind], known)
    memory[pl.ds(steps, SUBLANES), :] = known
    for copy in copies[3:8]:
        copy.wait()
    to_below = jnp.where(lane_of(first.shape) == 0, 0.0, v0 * first)[:, :padded]

    coeff = jnp.zeros(regime.shape, jnp.float32)
    for kind in range(rates.shape[1]):
        coeff = jnp.where(regime[...] == kind, rates[0, kind], coeff)
    on_land = land[...] == 1
    sea[...] = jnp.where(on_land, 0.0, coeff)
    fixed = jnp.where(on_land, coeff * land_temp[...], 0.0)

    count = width // LANES
    rest = pl.ds(lev * rows, (padded - lev) * rows)
    for k, cut in enumerate(tiles_of(width)):
        for l in range(lev):
            levels[k, pl.ds(l * rows, rows), :] = state[l, :, cut]
        levels[k, rest, :] = jnp.zeros((rest.size, LANES), jnp.float32)
        for t in range(steps):
            by_row[k, pl.ds(t * rows, rows), :] = guess[t, :, cut]
    for p in range(rows):
        for k, cut in enumerate(tiles_of(width)):
            own = levels[k, pl.ds(p, padded, stride=rows), :]
            below = jnp.dot(to_below, own, precision=EXACT, preferred_element_type=jnp.float32)
            part = below + fixed[p : p + 1, k * LANES : (k + 1) * LANES]
            base[p, :, cut] = part
            drive[p, :, cut] = part + sea[p : p + 1, cut] * by_row[k, pl.ds(p, steps, stride=rows), :]
    ship(drive, chunk, face)
    fields = jnp.concatenate([state[0], regime[...].astype(jnp.float32)], axis=0)
    for a, window in windows(lambda k: fields[:, k * LANES : (k + 1) * LANES], count, face):
        chunk[a, pl.ds(chunk.shape[1] - 2 * rows, 2 * rows), :] = window.astype(jnp.bfloat16)
    copies[8].wait()


def evolve(first, last, memory, arrived, fields, trace, *refs):
    if last:
        away, drive, past, packed, done = refs
    else:
        drive, past, packed = refs
    tiles, steps, cells = trace.shape
    grid_rows = fields.shape[1]
    rows = grid_rows // tiles
    face = cells // rows
    groups = steps // SUBLANES
    side = pl.ds(SUBLANES, grid_rows)
    if first:
        for a in range(tiles):
            both = arrived[a, pl.ds(arrived.shape[1] - 2 * rows, 2 * rows), :].astype(jnp.float32)
            fields[0, pl.ds(a * rows, rows), :] = both[:rows]
            fields[1, pl.ds(a * rows, rows), :] = both[rows:]
        regime = fields[1]
        coeff = jnp.zeros(regime.shape, jnp.float32)
        for kind in range(memory.shape[0] - steps - 2):
            coeff = jnp.where(regime == kind, memory[steps + 2 + kind : steps + 3 + kind, :], coeff)
        fields[1] = memory[steps : steps + 1, :] - coeff
    mix = memory[steps + 1 : steps + 2, :]
    edge = jnp.zeros((SUBLANES, LANES), jnp.float32)
    for n in range(steps + 1):
        past[n, pl.ds(0, SUBLANES), :] = edge
        past[n, pl.ds(SUBLANES + grid_rows, SUBLANES), :] = edge
    lane = lane_of((tiles, LANES))

    def west(x, by=1):
        return pltpu.roll(x, by, axis=1)

    def east(x, by=1):
        return pltpu.roll(x, LANES - by, axis=1)

    def weight(j):
        return memory[j : j + 1, :]

    def receive(g):
        for a in range(tiles):
            for p, tile in enumerate(landed(arrived, a, rows, face, g)):
                drive[g, pl.ds((a * rows + p) * SUBLANES, SUBLANES), :] = tile

    def known(n, upto):
        total = drive[n // SUBLANES, pl.ds(n % SUBLANES, grid_rows, stride=SUBLANES), :]
        for k in range(upto):
            total = total + weight(n - k) * past[k, side, :]
        return total

    def beside(n):
        return past[n, pl.ds(SUBLANES - 1, grid_rows), :] + past[n, pl.ds(SUBLANES + 1, grid_rows), :]

    def keep(n, surface):
        past[n, side, :] = surface
        if n == 0:
            return
        g, t = (n - 1) // SUBLANES, (n - 1) % SUBLANES
        for j in range(cells // LANES):
            even = past[n, pl.ds(SUBLANES + 2 * j, tiles, stride=rows), :]
            odd = past[n, pl.ds(SUBLANES + 2 * j + 1, tiles, stride=rows), :]
            packed[j, g, pl.ds(t, tiles, stride=SUBLANES), :] = pick(lane, (face,), (even, pltpu.roll(odd, face, axis=1)))
        if t == SUBLANES - 1:
            now = pl.ds(g * SUBLANES, SUBLANES)
            for j in range(cells // LANES):
                for a in range(tiles):
                    tile = packed[j, g, pl.ds(a * SUBLANES, SUBLANES), :]
                    trace[a, now, pl.ds(j * LANES, LANES)] = tile.astype(jnp.bfloat16)
            if last:
                pltpu.make_async_copy(trace.at[:, now, :], away.at[:, now, :], done.at[g]).start()

    surface = fields[0]
    receive(0)
    keep(0, surface)
    stay = fields[1]
    stay_west, stay_east = west(stay), east(stay)
    before = None
    for n in range(0, steps, 2):
        if n % SUBLANES == 0 and n // SUBLANES + 1 < groups:
            receive(n // SUBLANES + 1)
        part = known(n, max(n - 1, 0))
        here, at_west, at_east = part, west(part), east(part)
        if before is not None:
            here = here + weight(1) * before[0]
            at_west = at_west + weight(1) * before[1]
            at_east = at_east + weight(1) * before[2]
        rim = beside(n)
        w1, e1, w2, e2 = west(surface), east(surface), west(surface, 2), east(surface, 2)
        next_here = (stay * surface + here) + mix * (rim + (w1 + e1))
        next_west = (stay_west * w1 + at_west) + mix * (west(rim) + (w2 + surface))
        next_east = (stay_east * e1 + at_east) + mix * (east(rim) + (surface + e2))
        keep(n + 1, next_here)
        surface = (stay * next_here + known(n + 1, n + 1)) + mix * (beside(n + 1) + (next_west + next_east))
        keep(n + 2, surface)
        before = (next_here, next_west, next_east)
    if last:
        for g in range(groups):
            now = pl.ds(g * SUBLANES, SUBLANES)
            pltpu.make_async_copy(trace.at[:, now, :], away.at[:, now, :], done.at[g]).wait()


def product(trace, regrid, a):
    return lax.dot_general(trace[a], regrid[a], (((1,), (1,)), ((), ())), preferred_element_type=jnp.float32)


def redrive(trace, regrid, base, sea, chunk, drive):
    tiles, steps, cells = trace.shape
    rows, _, width = base.shape
    face = cells // rows
    count = width // LANES
    for k, cut in enumerate(tiles_of(width)):
        mapped = joined(product(trace, regrid, 2 * k), product(trace, regrid, 2 * k + 1), face)
        for p in range(rows):
            drive[p, :, cut] = base[p, :, cut] + sea[p : p + 1, cut] * mapped[p]
    ship(drive, chunk, face)


def remap(trace, regrid, forcing, by_row):
    tiles, steps, cells = trace.shape
    _, rows, width = forcing.shape
    face = cells // rows
    for k, cut in enumerate(tiles_of(width)):
        mapped = joined(product(trace, regrid, 2 * k), product(trace, regrid, 2 * k + 1), face)
        for p in range(rows):
            by_row[k, pl.ds(p, steps, stride=rows), :] = mapped[p]
        for t in range(steps):
            forcing[t, :, cut] = by_row[k, pl.ds(t * rows, rows), :]


def unforced(state, mats, rest, stack, levels, by_row):
    lev, rows, width = state.shape
    padded = mats.shape[1]
    fill = pl.ds(lev * rows, (padded - lev) * rows)
    still = mats[0][:, :padded]
    for k, cut in enumerate(tiles_of(width)):
        for l in range(lev):
            levels[k, pl.ds(l * rows, rows), :] = state[l, :, cut]
        levels[k, fill, :] = jnp.zeros((fill.size, LANES), jnp.float32)
        for p in range(rows):
            own = levels[k, pl.ds(p, padded, stride=rows), :]
            end = jnp.dot(still, own, precision=EXACT, preferred_element_type=jnp.float32)
            by_row[k, pl.ds(p, padded, stride=rows), :] = end
        for l in range(lev):
            rest[l, :, cut] = by_row[k, pl.ds(l * rows, rows), :]
    left = mats[1]
    for i in range(stack.shape[0]):
        part = left.astype(jnp.bfloat16)
        stack[i] = part
        left = left - part.astype(jnp.float32)


def finish(history, rest, stack, final, by_row):
    tiles, steps, cells = history.shape
    lev, rows, width = rest.shape
    padded = stack.shape[1]
    face = cells // rows
    for k, cut in enumerate(tiles_of(width)):
        seen = joined(history[2 * k].astype(jnp.float32), history[2 * k + 1].astype(jnp.float32), face)
        for p in range(rows):
            end = None
            for i in range(stack.shape[0]):
                part = jnp.dot(
                    stack[i][:, :steps], seen[p].astype(jnp.bfloat16), preferred_element_type=jnp.float32
                )
                end = part if end is None else end + part
            by_row[k, pl.ds(p, padded, stride=rows), :] = end
        for l in range(lev):
            final[l, :, cut] = rest[l, :, cut] + by_row[k, pl.ds(l * rows, rows), :]


def on_device(state, guess, regrid, regime, land, land_temp, exchange_rate, vertical, mixing):
    _, lev, rows, width = state.shape
    steps = guess.shape[1]
    tiles = lax.axis_size("tile")
    face = width // tiles
    cells = rows * face
    grid_rows = rows * tiles
    if 2 * face != LANES or LANES - face < 2 * steps or 2 * rows != SUBLANES or steps != 3 * SUBLANES:
        raise ValueError("unsupported sizes")
    padded = -(-lev // SUBLANES) * SUBLANES
    f32, bf16 = jnp.float32, jnp.bfloat16
    shape = jax.ShapeDtypeStruct
    state, guess, blocks = state[0], guess[0], regrid[0, 0]

    count = width // LANES
    by_row = shape((count, steps * rows, LANES), f32)
    levels = shape((count, padded * rows, LANES), f32)
    fields_shape = shape((2, grid_rows, LANES), f32)
    trace_shape = shape((tiles, steps, cells), bf16)
    groups = steps // SUBLANES
    sent = rows * steps * 3 // 4
    drive = shape((rows, steps, width), f32)
    stepping = [
        shape((groups, grid_rows * SUBLANES, LANES), f32),
        shape((steps + 1, grid_rows + 2 * SUBLANES, LANES), f32),
        shape((cells // LANES, groups, tiles * SUBLANES, LANES), f32),
    ]

    arrays = (exchange_rate, vertical, mixing[None], regime[0], land[0], land_temp[0], state, guess, blocks)
    near = [pltpu.SMEM(a.shape, a.dtype) for a in arrays[:3]] + [shape(a.shape, a.dtype) for a in arrays[3:8]]
    chunk, base, sea, mats, memory, blocks = run(
        prepare,
        (
            shape((tiles, sent + 2 * rows, LANES), bf16),
            shape((rows, steps, width), f32),
            shape((rows, width), f32),
            shape((2, padded, LANES), f32),
            shape((steps + SUBLANES, LANES), f32),
            shape(blocks.shape, blocks.dtype),
        ),
        arrays,
        [shape(((steps + 1) * padded, LANES), f32), by_row, levels, drive] + near + [pltpu.SemaphoreType.DMA((len(arrays),))],
        far=len(arrays),
    )
    for sweep in range(ITERS):
        arrived = lax.all_to_all(chunk, "tile", split_axis=0, concat_axis=0, tiled=True)
        if sweep == 0:
            fields, trace = run(
                functools.partial(evolve, True, False), (fields_shape, trace_shape), (memory, arrived), stepping
            )
        else:
            trace, away = run(
                functools.partial(evolve, False, True),
                (trace_shape, trace_shape),
                (memory, arrived, fields),
                stepping + [pltpu.SemaphoreType.DMA((groups,))],
                outward=1,
            )
        partner = lax.ppermute(trace, "mp", [(0, 1), (1, 0)])
        if sweep < ITERS - 1:
            chunk = run(
                redrive,
                shape((tiles, sent, LANES), bf16),
                (partner, blocks, base, sea),
                [drive],
            )
    history = lax.all_to_all(away, "tile", split_axis=0, concat_axis=0, tiled=True)
    forcing = run(remap, shape((steps, rows, width), f32), (partner, blocks), [by_row])
    final_shape = shape((lev, rows, width), f32)
    rest, stack = run(unforced, (final_shape, shape((3, padded, LANES), bf16)), (state, mats), [levels, levels])
    final = run(finish, final_shape, (history, rest, stack), [levels])
    return final[None], forcing[None]


def solution(mesh):
    return jax.shard_map(
        on_device,
        mesh=mesh,
        in_specs=(
            P("mp", None, "tile", None),
            P("mp", None, "tile", None),
            P("mp", "tile", None, None, None),
            P("mp", "tile", None),
            P("mp", "tile", None),
            P("mp", "tile", None),
            P("mp", None),
            P("mp", None),
            P("mp"),
        ),
        out_specs=(P("mp", None, "tile", None), P("mp", None, "tile", None)),
        check_vma=False,
    )
```

```python
import functools
import math

import jax
import jax.numpy as jnp
from jax import lax
from jax.experimental import pallas as pl
from jax.experimental.pallas import tpu as pltpu
from jax.sharding import PartitionSpec as P

ITERS = 2
LANES = 128
SUBLANES = 8
SPARE = 4 << 20
EXACT = lax.Precision.HIGHEST
VMEM = pl.BlockSpec(memory_space=pltpu.VMEM)
HBM = pl.BlockSpec(memory_space=pltpu.HBM)


def size_of(leaf):
    if len(leaf.shape) < 2:
        return 4096
    rows = -(-leaf.shape[-2] // SUBLANES) * SUBLANES
    lanes = -(-leaf.shape[-1] // LANES) * LANES
    return math.prod(leaf.shape[:-2]) * rows * lanes * 4


def run(kernel, out, arrays, scratch, far=0, outward=0, cost=1):
    leaves = jax.tree.leaves(out) + list(arrays[far:]) + [leaf for leaf in scratch if isinstance(leaf, jax.ShapeDtypeStruct)]
    return pl.pallas_call(
        kernel,
        out_shape=out,
        in_specs=[HBM] * far + [VMEM] * (len(arrays) - far),
        out_specs=(VMEM,) * (len(out) - outward) + (HBM,) * outward if isinstance(out, tuple) else (HBM if outward else VMEM),
        scratch_shapes=[leaf if not isinstance(leaf, jax.ShapeDtypeStruct) else pltpu.VMEM(leaf.shape, leaf.dtype) for leaf in scratch],
        compiler_params=pltpu.CompilerParams(vmem_limit_bytes=sum(map(size_of, leaves)) + SPARE),
        cost_estimate=pl.CostEstimate(flops=cost * 1000000, bytes_accessed=0, transcendentals=0),
        name=getattr(kernel, "__name__", "evolve"),
    )(*[pltpu.with_memory_space_constraint(a, pltpu.HBM) for a in arrays[:far]], *arrays[far:])


def lane_of(shape):
    return lax.broadcasted_iota(jnp.int32, shape, len(shape) - 1)


def row_of(shape):
    return lax.broadcasted_iota(jnp.int32, shape, 0)


def tiles_of(width):
    return [pl.ds(k * LANES, LANES) for k in range(width // LANES)]


def windows(tile, count, face):
    half = (LANES - face) // 2
    for k in range(count):
        own, left, right = tile(k), tile((k - 1) % count), tile((k + 1) % count)
        lane = lane_of(own.shape)
        yield 2 * k, jnp.where(lane < face + half, own, left)
        yield 2 * k + 1, pltpu.roll(jnp.where(lane < half, right, own), face, axis=1)


def pick(lane, cuts, parts):
    out = parts[-1]
    for cut, part in zip(reversed(cuts), reversed(parts[:-1])):
        out = jnp.where(lane < cut, part, out)
    return out


def ship(drive, chunk, face):
    rows, steps, width = drive.shape
    lane = lane_of((SUBLANES, LANES))
    views = [windows(lambda k, p=p: drive[p, :, k * LANES : (k + 1) * LANES], width // LANES, face) for p in range(rows)]
    for group in zip(*views):
        early, middle, late = [[view[g * SUBLANES : (g + 1) * SUBLANES] for _, view in group] for g in range(3)]
        tiles = []
        for p in range(rows):
            near, far = pltpu.roll(late[p], 24, axis=1), pltpu.roll(late[p], LANES - 24, axis=1)
            tiles.append(pick(lane, (88, 96, 104), (early[p], near, far, early[p])))
        for p in range(0, rows, 2):
            near, far = pltpu.roll(middle[p + 1], 16, axis=1), pltpu.roll(middle[p + 1], LANES - 16, axis=1)
            tiles.append(pick(lane, (80, 96, 112), (middle[p], near, far, middle[p])))
        rest = middle[1::2] + late
        for first, second in zip(rest[::2], rest[1::2]):
            tiles.append(pick(lane, (face,), (first, pltpu.roll(second, face, axis=1))))
        for i, tile in enumerate(tiles):
            chunk[group[0][0], pl.ds(i * SUBLANES, SUBLANES), :] = tile.astype(jnp.bfloat16)


def landed(arrived, a, rows, face, g):
    lane = lane_of((SUBLANES, LANES))
    tile = lambda i: arrived[a, pl.ds(i * SUBLANES, SUBLANES), :].astype(jnp.float32)
    if g == 0:
        return [tile(p) for p in range(rows)]

    def rest(i):
        held = tile(rows + rows // 2 + i // 2)
        return pltpu.roll(held, face, axis=1) if i % 2 else held

    if g == 1:
        out = []
        for p in range(0, rows, 2):
            both = tile(rows + p // 2)
            near, far = pltpu.roll(both, LANES - 16, axis=1), pltpu.roll(both, 16, axis=1)
            out += [both, pick(lane, (face, 96), (rest(p // 2), near, far))]
        return out
    out = []
    for p in range(rows):
        both = tile(p)
        near, far = pltpu.roll(both, LANES - 24, axis=1), pltpu.roll(both, 24, axis=1)
        out.append(pick(lane, (face, 96), (rest(rows // 2 + p), near, far)))
    return out


def joined(first, second, face):
    out = []
    for j in range(first.shape[1] // LANES):
        cut = slice(j * LANES, (j + 1) * LANES)
        x, y = first[:, cut], second[:, cut]
        lane = lane_of(x.shape)
        out.append(jnp.where(lane < face, x, pltpu.roll(y, face, axis=1)))
        out.append(jnp.where(lane < face, pltpu.roll(x, face, axis=1), y))
    return out


def prepare(
    rates_far, vertical_far, regime_far, land_far, land_temp_far, state_far, guess_far,
    chunk, base, sea, memory, xs,
    by_row, levels, drive, rates, vertical, regime, land, land_temp, state, guess, done,
):
    pairs = (
        (rates_far, rates),
        (vertical_far, vertical),
        (regime_far, regime),
        (land_far, land),
        (land_temp_far, land_temp),
        (state_far, state),
        (guess_far, guess),
    )
    copies = [pltpu.make_async_copy(far, near, done.at[i]) for i, (far, near) in enumerate(pairs)]
    for copy in copies:
        copy.start()
    for copy in copies[:2]:
        copy.wait()
    lev, rows, width = state.shape
    steps = guess.shape[0]
    padded = xs.shape[1]
    deep = levels.shape[1] // rows
    face = width // chunk.shape[0]

    shape = (padded, LANES)
    row, lane = row_of(shape), lane_of(shape)
    up = jnp.zeros(shape, jnp.float32)
    down = jnp.zeros(shape, jnp.float32)
    for l in range(lev - 1):
        up = jnp.where((row == l) & (row > 0), vertical[0, l], up)
        down = jnp.where(row == l + 1, vertical[0, l], down)
    keep = jnp.where(row == 0, 0.0, 1.0 - up - down)
    power = jnp.where((row == lane) & (row < lev), 1.0, 0.0)
    first = jnp.zeros((steps, LANES), jnp.float32)
    for n in range(steps + 1):
        xs[n] = power
        if n == steps:
            break
        first = jnp.where(row_of(first.shape) == n, power[1:2, :], first)
        power = keep * power + up * pltpu.roll(power, padded - 1, axis=0) + down * pltpu.roll(power, 1, axis=0)
    v0 = vertical[0, 0]
    memory[pl.ds(0, steps), :] = jnp.broadcast_to(v0 * first[:, 0:1], first.shape)
    shape = (SUBLANES, LANES)
    row = row_of(shape)
    known = jnp.full(shape, v0, jnp.float32)
    for kind in range(rates.shape[1]):
        known = jnp.where(row == 1 + kind, rates[0, kind], known)
    memory[pl.ds(steps, SUBLANES), :] = known
    for copy in copies[2:]:
        copy.wait()
    to_below = jnp.where(lane_of(first.shape) == 0, 0.0, v0 * first)
    high = to_below.astype(jnp.bfloat16).astype(jnp.float32)
    low = to_below - high
    lane = lane_of(first.shape)
    to_below = pick(lane, (deep, 2 * deep), (high, pltpu.roll(high, deep, axis=1), pltpu.roll(low, 2 * deep, axis=1)))
    to_below = to_below[:, : 3 * deep].astype(jnp.bfloat16)

    coeff = jnp.zeros(regime.shape, jnp.float32)
    for kind in range(rates.shape[1]):
        coeff = jnp.where(regime[...] == kind, rates[0, kind], coeff)
    on_land = land[...] == 1
    sea[...] = jnp.where(on_land, 0.0, coeff)
    fixed = jnp.where(on_land, coeff * land_temp[...], 0.0)

    count = width // LANES
    rest = pl.ds(lev * rows, (deep - lev) * rows)
    for k, cut in enumerate(tiles_of(width)):
        for l in range(lev):
            levels[k, pl.ds(l * rows, rows), :] = state[l, :, cut]
        levels[k, rest, :] = jnp.zeros((rest.size, LANES), jnp.float32)
        for t in range(steps):
            by_row[k, pl.ds(t * rows, rows), :] = guess[t, :, cut]
    for p in range(rows):
        for k in range(0, count, 2):
            parts = []
            for i in (k, k + 1):
                own = levels[i, pl.ds(p, deep, stride=rows), :]
                near = own.astype(jnp.bfloat16)
                parts.append(jnp.concatenate([near, (own - near.astype(jnp.float32)).astype(jnp.bfloat16), near], axis=0))
            pair = jnp.dot(to_below, jnp.concatenate(parts, axis=1), preferred_element_type=jnp.float32)
            for i in (k, k + 1):
                cut = pl.ds(i * LANES, LANES)
                part = pair[:, (i - k) * LANES : (i - k + 1) * LANES] + fixed[p : p + 1, i * LANES : (i + 1) * LANES]
                base[p, :, cut] = part
                drive[p, :, cut] = part + sea[p : p + 1, cut] * by_row[i, pl.ds(p, steps, stride=rows), :]
    ship(drive, chunk, face)
    fields = jnp.concatenate([state[0], regime[...].astype(jnp.float32)], axis=0)
    for a, window in windows(lambda k: fields[:, k * LANES : (k + 1) * LANES], count, face):
        chunk[a, pl.ds(chunk.shape[1] - 2 * rows, 2 * rows), :] = window.astype(jnp.bfloat16)


def evolve(first, last, *refs):
    if first:
        blocks_far, mixing, memory, arrived, fields, trace, blocks, drive, past, packed, fetched = refs
        fetch = pltpu.make_async_copy(blocks_far, blocks, fetched)
        fetch.start()
    else:
        memory, arrived, fields, trace, away, drive, past, packed, done = refs
    tiles, steps, cells = trace.shape
    grid_rows = fields.shape[1]
    rows = grid_rows // tiles
    face = cells // rows
    groups = steps // SUBLANES
    side = pl.ds(SUBLANES, grid_rows)
    if first:
        for a in range(tiles):
            both = arrived[a, pl.ds(arrived.shape[1] - 2 * rows, 2 * rows), :].astype(jnp.float32)
            fields[0, pl.ds(a * rows, rows), :] = both[:rows]
            fields[1, pl.ds(a * rows, rows), :] = both[rows:]
        regime = fields[1]
        coeff = jnp.zeros(regime.shape, jnp.float32)
        for kind in range(memory.shape[0] - steps - 1):
            coeff = jnp.where(regime == kind, memory[steps + 1 + kind : steps + 2 + kind, :], coeff)
        mix = jnp.broadcast_to(mixing[...].reshape(1, 1), coeff.shape)
        fields[1] = 1.0 - memory[steps : steps + 1, :] - coeff - 4.0 * mix
        fields[2] = mix
    mix = fields[2, 0:1, :]
    edge = jnp.zeros((SUBLANES, LANES), jnp.float32)
    for n in range(steps + 1):
        past[n, pl.ds(0, SUBLANES), :] = edge
        past[n, pl.ds(SUBLANES + grid_rows, SUBLANES), :] = edge
    lane = lane_of((tiles, LANES))

    def west(x, by=1):
        return pltpu.roll(x, by, axis=1)

    def east(x, by=1):
        return pltpu.roll(x, LANES - by, axis=1)

    def weight(j):
        return memory[j : j + 1, :]

    def receive(g):
        for a in range(tiles):
            for p, tile in enumerate(landed(arrived, a, rows, face, g)):
                drive[g, pl.ds((a * rows + p) * SUBLANES, SUBLANES), :] = tile

    def known(n, upto):
        total = drive[n // SUBLANES, pl.ds(n % SUBLANES, grid_rows, stride=SUBLANES), :]
        for k in range(upto):
            total = total + weight(n - k) * past[k, side, :]
        return total

    def beside(n):
        return past[n, pl.ds(SUBLANES - 1, grid_rows), :] + past[n, pl.ds(SUBLANES + 1, grid_rows), :]

    def keep(n, surface):
        past[n, side, :] = surface
        if n == 0:
            return
        g, t = (n - 1) // SUBLANES, (n - 1) % SUBLANES
        for j in range(cells // LANES):
            even = past[n, pl.ds(SUBLANES + 2 * j, tiles, stride=rows), :]
            odd = past[n, pl.ds(SUBLANES + 2 * j + 1, tiles, stride=rows), :]
            packed[j, g, pl.ds(t, tiles, stride=SUBLANES), :] = pick(lane, (face,), (even, pltpu.roll(odd, face, axis=1)))
        if t == SUBLANES - 1:
            now = pl.ds(g * SUBLANES, SUBLANES)
            for j in range(cells // LANES):
                for a in range(tiles):
                    tile = packed[j, g, pl.ds(a * SUBLANES, SUBLANES), :]
                    trace[a, now, pl.ds(j * LANES, LANES)] = tile.astype(jnp.bfloat16)
            if last:
                pltpu.make_async_copy(trace.at[:, now, :], away.at[:, now, :], done.at[g]).start()

    surface = fields[0]
    receive(0)
    keep(0, surface)
    stay = fields[1]
    for n in range(0, steps, 2):
        if n % SUBLANES == 0 and n // SUBLANES + 1 < groups:
            receive(n // SUBLANES + 1)
        still = (stay * surface + known(n, n)) + mix * beside(n)
        middle = still + mix * (west(surface) + east(surface))
        twice = (west(surface, 2) + east(surface, 2)) + (surface + surface)
        sides = (west(still) + east(still)) + mix * twice
        keep(n + 1, middle)
        surface = (stay * middle + known(n + 1, n + 1)) + mix * (beside(n + 1) + sides)
        keep(n + 2, surface)
    if last:
        for g in range(groups):
            now = pl.ds(g * SUBLANES, SUBLANES)
            pltpu.make_async_copy(trace.at[:, now, :], away.at[:, now, :], done.at[g]).wait()
    if first:
        fetch.wait()


def product(trace, regrid, a):
    return lax.dot_general(trace[a], regrid[a], (((1,), (1,)), ((), ())), preferred_element_type=jnp.float32)


def redrive(trace, regrid, base, sea, chunk, drive):
    tiles, steps, cells = trace.shape
    rows, _, width = base.shape
    face = cells // rows
    count = width // LANES
    for k, cut in enumerate(tiles_of(width)):
        mapped = joined(product(trace, regrid, 2 * k), product(trace, regrid, 2 * k + 1), face)
        for p in range(rows):
            drive[p, :, cut] = base[p, :, cut] + sea[p : p + 1, cut] * mapped[p]
    ship(drive, chunk, face)


def remap(trace, regrid, forcing, by_row):
    tiles, steps, cells = trace.shape
    _, rows, width = forcing.shape
    face = cells // rows
    for k, cut in enumerate(tiles_of(width)):
        mapped = joined(product(trace, regrid, 2 * k), product(trace, regrid, 2 * k + 1), face)
        for p in range(rows):
            by_row[k, pl.ds(p, steps, stride=rows), :] = mapped[p]
        for t in range(steps):
            forcing[t, :, cut] = by_row[k, pl.ds(t * rows, rows), :]


def unforced(state, powers, rest, stack, levels, by_row):
    lev, rows, width = state.shape
    padded = powers.shape[1]
    steps = powers.shape[0] - 1
    fill = pl.ds(lev * rows, (padded - lev) * rows)
    row, lane = row_of(powers.shape[1:]), lane_of(powers.shape[1:])
    still = jnp.where(row == 0, 0.0, powers[steps])[:, :padded]
    for k, cut in enumerate(tiles_of(width)):
        for l in range(lev):
            levels[k, pl.ds(l * rows, rows), :] = state[l, :, cut]
        levels[k, fill, :] = jnp.zeros((fill.size, LANES), jnp.float32)
        for p in range(rows):
            own = levels[k, pl.ds(p, padded, stride=rows), :]
            end = jnp.dot(still, own, precision=EXACT, preferred_element_type=jnp.float32)
            by_row[k, pl.ds(p, padded, stride=rows), :] = end
        for l in range(lev):
            rest[l, :, cut] = by_row[k, pl.ds(l * rows, rows), :]
    left = jnp.zeros(row.shape, jnp.float32)
    for n in range(steps):
        left = jnp.where(lane == steps - 1 - n, powers[n][:, 0:1], left)
    for i in range(stack.shape[0]):
        part = left.astype(jnp.bfloat16)
        stack[i] = part
        left = left - part.astype(jnp.float32)


def finish(history, rest, stack, final_far, final, by_row, done):
    tiles, steps, cells = history.shape
    lev, rows, width = rest.shape
    padded = stack.shape[1]
    face = cells // rows
    for k, cut in enumerate(tiles_of(width)):
        seen = joined(history[2 * k].astype(jnp.float32), history[2 * k + 1].astype(jnp.float32), face)
        for p in range(rows):
            end = None
            for i in range(stack.shape[0]):
                part = jnp.dot(
                    stack[i][:, :steps], seen[p].astype(jnp.bfloat16), preferred_element_type=jnp.float32
                )
                end = part if end is None else end + part
            by_row[k, pl.ds(p, padded, stride=rows), :] = end
        for l in range(lev):
            final[k, l] = rest[l, :, cut] + by_row[k, pl.ds(l * rows, rows), :]
        pltpu.make_async_copy(final.at[k], final_far.at[:, :, cut], done.at[k]).start()
    for k, cut in enumerate(tiles_of(width)):
        pltpu.make_async_copy(final.at[k], final_far.at[:, :, cut], done.at[k]).wait()


def on_device(state, guess, regrid, regime, land, land_temp, exchange_rate, vertical, mixing):
    _, lev, rows, width = state.shape
    steps = guess.shape[1]
    tiles = lax.axis_size("tile")
    face = width // tiles
    cells = rows * face
    grid_rows = rows * tiles
    if 2 * face != LANES or LANES - face < 2 * steps or 2 * rows != SUBLANES or steps != 3 * SUBLANES:
        raise ValueError("unsupported sizes")
    padded = -(-lev // SUBLANES) * SUBLANES
    f32, bf16 = jnp.float32, jnp.bfloat16
    shape = jax.ShapeDtypeStruct
    state, guess, blocks = state[0], guess[0], regrid[0, 0]

    count = width // LANES
    by_row = shape((count, steps * rows, LANES), f32)
    levels = shape((count, padded * rows, LANES), f32)
    fields_shape = shape((3, grid_rows, LANES), f32)
    trace_shape = shape((tiles, steps, cells), bf16)
    groups = steps // SUBLANES
    sent = rows * steps * 3 // 4
    drive = shape((rows, steps, width), f32)
    stepping = [
        shape((groups, grid_rows * SUBLANES, LANES), f32),
        shape((steps + 1, grid_rows + 2 * SUBLANES, LANES), f32),
        shape((cells // LANES, groups, tiles * SUBLANES, LANES), f32),
    ]

    arrays = (exchange_rate, vertical, regime[0], land[0], land_temp[0], state, guess)
    near = [pltpu.SMEM(a.shape, a.dtype) for a in arrays[:2]] + [shape(a.shape, a.dtype) for a in arrays[2:]]
    chunk, base, sea, memory, powers = run(
        prepare,
        (
            shape((tiles, sent + 2 * rows, LANES), bf16),
            shape((rows, steps, width), f32),
            shape((rows, width), f32),
            shape((steps + SUBLANES, LANES), f32),
            shape((steps + 1, padded, LANES), f32),
        ),
        arrays,
        [by_row, shape((count, 4 * SUBLANES * rows, LANES), f32), drive] + near + [pltpu.SemaphoreType.DMA((len(arrays),))],
        far=len(arrays),
    )
    for sweep in range(ITERS):
        arrived = lax.all_to_all(chunk, "tile", split_axis=0, concat_axis=0, tiled=True)
        if sweep == 0:
            fields, trace, blocks = run(
                functools.partial(evolve, True, False),
                (fields_shape, trace_shape, shape(blocks.shape, blocks.dtype)),
                (blocks, mixing, memory, arrived),
                stepping + [pltpu.SemaphoreType.DMA(())],
                far=1,
            )
        else:
            trace, away = run(
                functools.partial(evolve, False, True),
                (trace_shape, trace_shape),
                (memory, arrived, fields),
                stepping + [pltpu.SemaphoreType.DMA((groups,))],
                outward=1,
            )
        partner = lax.ppermute(trace, "mp", [(0, 1), (1, 0)])
        if sweep < ITERS - 1:
            chunk = run(
                redrive,
                shape((tiles, sent, LANES), bf16),
                (partner, blocks, base, sea),
                [drive],
            )
    history = lax.all_to_all(away, "tile", split_axis=0, concat_axis=0, tiled=True)
    forcing = run(remap, shape((steps, rows, width), f32), (partner, blocks), [by_row])
    final_shape = shape((lev, rows, width), f32)
    rest, stack = run(unforced, (final_shape, shape((3, padded, LANES), bf16)), (state, powers), [levels, levels])
    final = run(
        finish,
        final_shape,
        (history, rest, stack),
        [shape((count, lev, rows, LANES), f32), levels, pltpu.SemaphoreType.DMA((count,))],
        outward=1,
    )
    return final[None], forcing[None]


def solution(mesh):
    return jax.shard_map(
        on_device,
        mesh=mesh,
        in_specs=(
            P("mp", None, "tile", None),
            P("mp", None, "tile", None),
            P("mp", "tile", None, None, None),
            P("mp", "tile", None),
            P("mp", "tile", None),
            P("mp", "tile", None),
            P("mp", None),
            P("mp", None),
            P("mp"),
        ),
        out_specs=(P("mp", None, "tile", None), P("mp", None, "tile", None)),
        check_vma=False,
    )
```

```python
import functools
import math

import jax
import jax.numpy as jnp
from jax import lax
from jax.experimental import pallas as pl
from jax.experimental.pallas import tpu as pltpu
from jax.sharding import PartitionSpec as P

ITERS = 2
LANES = 128
SUBLANES = 8
SPARE = 4 << 20
EXACT = lax.Precision.HIGHEST
VMEM = pl.BlockSpec(memory_space=pltpu.VMEM)
HBM = pl.BlockSpec(memory_space=pltpu.HBM)


def size_of(leaf):
    if len(leaf.shape) < 2:
        return 4096
    rows = -(-leaf.shape[-2] // SUBLANES) * SUBLANES
    lanes = -(-leaf.shape[-1] // LANES) * LANES
    return math.prod(leaf.shape[:-2]) * rows * lanes * 4


def run(kernel, out, arrays, scratch, far=0, outward=0, cost=1):
    leaves = jax.tree.leaves(out) + list(arrays[far:]) + [leaf for leaf in scratch if isinstance(leaf, jax.ShapeDtypeStruct)]
    return pl.pallas_call(
        kernel,
        out_shape=out,
        in_specs=[HBM] * far + [VMEM] * (len(arrays) - far),
        out_specs=(VMEM,) * (len(out) - outward) + (HBM,) * outward if isinstance(out, tuple) else (HBM if outward else VMEM),
        scratch_shapes=[leaf if not isinstance(leaf, jax.ShapeDtypeStruct) else pltpu.VMEM(leaf.shape, leaf.dtype) for leaf in scratch],
        compiler_params=pltpu.CompilerParams(vmem_limit_bytes=sum(map(size_of, leaves)) + SPARE),
        cost_estimate=pl.CostEstimate(flops=cost * 1000000, bytes_accessed=0, transcendentals=0),
        name=getattr(kernel, "__name__", "evolve"),
    )(*[a if a.size == 1 else pltpu.with_memory_space_constraint(a, pltpu.HBM) for a in arrays[:far]], *arrays[far:])


def lane_of(shape):
    return lax.broadcasted_iota(jnp.int32, shape, len(shape) - 1)


def row_of(shape):
    return lax.broadcasted_iota(jnp.int32, shape, 0)


def tiles_of(width):
    return [pl.ds(k * LANES, LANES) for k in range(width // LANES)]


def windows(tile, count, face):
    half = (LANES - face) // 2
    for k in range(count):
        own, left, right = tile(k), tile((k - 1) % count), tile((k + 1) % count)
        lane = lane_of(own.shape)
        yield 2 * k, jnp.where(lane < face + half, own, left)
        yield 2 * k + 1, pltpu.roll(jnp.where(lane < half, right, own), face, axis=1)


def exchanged(x, y, face):
    lane = lane_of(x.shape)
    return (
        jnp.where(lane < face, x, pltpu.roll(y, face, axis=1)),
        jnp.where(lane < face, pltpu.roll(x, face, axis=1), y),
    )


def joined(first, second, face):
    out = []
    for j in range(first.shape[1] // LANES):
        cut = slice(j * LANES, (j + 1) * LANES)
        out += exchanged(first[:, cut], second[:, cut], face)
    return out


def pick(lane, cuts, parts):
    out = parts[-1]
    for cut, part in zip(reversed(cuts), reversed(parts[:-1])):
        out = jnp.where(lane < cut, part, out)
    return out


def turn(x, by):
    return pltpu.roll(x, by % LANES, axis=1)


def ship(drive, chunk, face):
    tiles, pairs, _, _ = drive.shape
    lane = lane_of((SUBLANES, LANES)) % face
    for a in range(tiles):
        own, halo = {}, {}
        for j in range(pairs):
            for g in range(3):
                now = pl.ds(g * SUBLANES, SUBLANES)
                own[j, g] = drive[a, j, now, :]
                halo[j, g] = pick(lane, (face // 2,), (drive[(a + 1) % tiles, j, now, :], drive[(a - 1) % tiles, j, now, :]))
        out = [own[j, g] for j in range(pairs) for g in range(3)]
        for j in range(pairs):
            out.append(pick(lane, (24, 32, 40), (halo[j, 0], turn(halo[j, 2], 24), turn(halo[j, 2], -24), halo[j, 0])))
        out.append(pick(lane, (16, 32, 48), (halo[0, 1], turn(halo[1, 1], 16), turn(halo[1, 1], -16), halo[0, 1])))
        for i, tile in enumerate(out):
            chunk[a, pl.ds(i * SUBLANES, SUBLANES), :] = tile.astype(jnp.bfloat16)


def landed(arrived, a, face, g):
    lane = lane_of((SUBLANES, LANES))
    tile = lambda i: arrived[a, pl.ds(i * SUBLANES, SUBLANES), :].astype(jnp.float32)
    out = []
    for j in range(2):
        main = tile(3 * j + g)
        halo = tile(8) if g == 1 else tile(6 + j)
        if g == 0 or (g, j) == (1, 0):
            out.append(pick(lane, (face,), (main, turn(halo, face))))
            out.append(pick(lane, (face,), (turn(main, face), halo)))
        else:
            by = 16 if g == 1 else 24
            out.append(pick(lane, (face, 96), (main, turn(halo, face - by), turn(halo, face + by))))
            out.append(pick(lane, (face, 96), (turn(main, face), turn(halo, -by), turn(halo, by))))
    return out


def prepare(
    rates_far, vertical_far, mixing_far, regime_far, land_far, land_temp_far, state_far, guess_far, blocks_far,
    chunk, base, sea, memory, xs, blocks,
    by_row, levels, drive, rates, vertical, mixing, regime, land, land_temp, state, guess, done,
):
    pairs = (
        (rates_far, rates),
        (vertical_far, vertical),
        (mixing_far, mixing),
        (regime_far, regime),
        (land_far, land),
        (land_temp_far, land_temp),
        (state_far, state),
        (guess_far, guess),
        (blocks_far.at[pl.ds(0, blocks.shape[0])], blocks),
    )
    copies = [pltpu.make_async_copy(far, near, done.at[i]) for i, (far, near) in enumerate(pairs)]
    for copy in copies:
        copy.start()
    for copy in copies[:3]:
        copy.wait()
    lev, rows, width = state.shape
    steps = guess.shape[0]
    padded = xs.shape[1]
    deep = levels.shape[1] // rows
    face = width // chunk.shape[0]

    shape = (padded, LANES)
    row, lane = row_of(shape), lane_of(shape)
    up = jnp.zeros(shape, jnp.float32)
    down = jnp.zeros(shape, jnp.float32)
    for l in range(lev - 1):
        up = jnp.where((row == l) & (row > 0), vertical[0, l], up)
        down = jnp.where(row == l + 1, vertical[0, l], down)
    keep = jnp.where(row == 0, 0.0, 1.0 - up - down)
    power = jnp.where((row == lane) & (row < lev), 1.0, 0.0)
    first = jnp.zeros((steps, LANES), jnp.float32)
    for n in range(steps + 1):
        xs[n] = power
        if n == steps:
            break
        first = jnp.where(row_of(first.shape) == n, power[1:2, :], first)
        power = keep * power + up * pltpu.roll(power, padded - 1, axis=0) + down * pltpu.roll(power, 1, axis=0)
    v0 = vertical[0, 0]
    memory[pl.ds(0, steps), :] = jnp.broadcast_to(v0 * first[:, 0:1], first.shape)
    shape = (SUBLANES, LANES)
    row = row_of(shape)
    known = jnp.where(row == 0, 1.0 - v0 - 4.0 * mixing[0, 0], mixing[0, 0])
    for kind in range(rates.shape[1]):
        known = jnp.where(row == 2 + kind, rates[0, kind], known)
    memory[pl.ds(steps, SUBLANES), :] = known
    for copy in copies[3:-1]:
        copy.wait()
    own_cell = (lane_of(first.shape) == 0) & (row_of(first.shape) == 0)
    to_below = jnp.where(own_cell, 1.0 - v0 - 4.0 * mixing[0, 0], v0 * first)
    high = to_below.astype(jnp.bfloat16).astype(jnp.float32)
    low = to_below - high
    lane = lane_of(first.shape)
    to_below = pick(lane, (deep, 2 * deep), (high, pltpu.roll(high, deep, axis=1), pltpu.roll(low, 2 * deep, axis=1)))
    to_below = to_below[:, : 3 * deep].astype(jnp.bfloat16)

    coeff = jnp.zeros(regime.shape, jnp.float32)
    for kind in range(rates.shape[1]):
        coeff = jnp.where(regime[...] == kind, rates[0, kind], coeff)
    on_land = land[...] == 1
    open_sea = jnp.where(on_land, 0.0, coeff)
    fixed = jnp.where(on_land, coeff * land_temp[...], 0.0)
    left = state[0] - state[0].astype(jnp.bfloat16).astype(jnp.float32)
    taken = coeff * left

    count = width // LANES
    rest = pl.ds(lev * rows, (deep - lev) * rows)
    for k, cut in enumerate(tiles_of(width)):
        levels[k, pl.ds(0, rows), :] = left[:, k * LANES : (k + 1) * LANES]
        for l in range(1, lev):
            levels[k, pl.ds(l * rows, rows), :] = state[l, :, cut]
        levels[k, rest, :] = jnp.zeros((rest.size, LANES), jnp.float32)
        for t in range(steps):
            by_row[k, pl.ds(t * rows, rows), :] = guess[t, :, cut]
    def below(p, k):
        parts = []
        for i in (k, k + 1):
            own = levels[i, pl.ds(p, deep, stride=rows), :]
            near = own.astype(jnp.bfloat16)
            parts.append(jnp.concatenate([near, (own - near.astype(jnp.float32)).astype(jnp.bfloat16), near], axis=0))
        pair = jnp.dot(to_below, jnp.concatenate(parts, axis=1), preferred_element_type=jnp.float32)
        return pair[:, :LANES], pair[:, LANES:]

    for j in range(rows // 2):
        two = (2 * j, 2 * j + 1)
        for k in range(0, count, 2):
            for i, *parts in zip((k, k + 1), *[below(p, k) for p in two]):
                cut = slice(i * LANES, (i + 1) * LANES)
                start = row_of(parts[0].shape) == 0
                still = [part + jnp.where(start, fixed[p : p + 1, cut] - taken[p : p + 1, cut], fixed[p : p + 1, cut]) for p, part in zip(two, parts)]
                slopes = [open_sea[p : p + 1, cut] for p in two]
                forced = [
                    part + slope * by_row[i, pl.ds(p, steps, stride=rows), :] for p, part, slope in zip(two, still, slopes)
                ]
                for b, tile in enumerate(exchanged(*still, face)):
                    base[2 * i + b, j] = tile
                for b, tile in enumerate(exchanged(*forced, face)):
                    drive[2 * i + b, j] = tile
                for b, tile in enumerate(exchanged(*slopes, face)):
                    sea[pl.ds((2 * i + b) * (rows // 2) + j, 1), :] = tile
    ship(drive, chunk, face)
    fields = jnp.concatenate([state[0], regime[...].astype(jnp.float32)], axis=0)
    for a, window in windows(lambda k: fields[:, k * LANES : (k + 1) * LANES], count, face):
        chunk[a, pl.ds(chunk.shape[1] - 2 * rows, 2 * rows), :] = window.astype(jnp.bfloat16)
    copies[-1].wait()


def evolve(first, last, *refs):
    if first:
        blocks_far, memory, arrived, fields, trace, blocks, drive, past, packed, fetched = refs
        half = blocks.shape[0]
        fetch = pltpu.make_async_copy(blocks_far.at[pl.ds(half, half)], blocks, fetched)
        fetch.start()
    else:
        memory, arrived, fields, trace, away, drive, past, packed, done = refs
    tiles, steps, cells = trace.shape
    grid_rows = fields.shape[1]
    rows = grid_rows // tiles
    face = cells // rows
    groups = steps // SUBLANES
    side = pl.ds(SUBLANES, grid_rows)
    if first:
        for a in range(tiles):
            both = arrived[a, pl.ds(arrived.shape[1] - 2 * rows, 2 * rows), :].astype(jnp.float32)
            fields[0, pl.ds(a * rows, rows), :] = both[:rows]
            fields[1, pl.ds(a * rows, rows), :] = both[rows:]
        regime = fields[1]
        coeff = jnp.zeros(regime.shape, jnp.float32)
        for kind in range(memory.shape[0] - steps - 2):
            coeff = jnp.where(regime == kind, memory[steps + 2 + kind : steps + 3 + kind, :], coeff)
        fields[1] = memory[steps : steps + 1, :] - coeff
    mix = memory[steps + 1 : steps + 2, :]
    edge = jnp.zeros((SUBLANES, LANES), jnp.float32)
    for n in range(steps + 1):
        past[n, pl.ds(0, SUBLANES), :] = edge
        past[n, pl.ds(SUBLANES + grid_rows, SUBLANES), :] = edge
    lane = lane_of((tiles, LANES))

    def west(x, by=1):
        return pltpu.roll(x, by, axis=1)

    def east(x, by=1):
        return pltpu.roll(x, LANES - by, axis=1)

    def weight(j):
        return memory[j : j + 1, :]

    def receive(g):
        for a in range(tiles):
            for p, tile in enumerate(landed(arrived, a, face, g)):
                drive[g, pl.ds((a * rows + p) * SUBLANES, SUBLANES), :] = tile

    def known(n, upto):
        total = drive[n // SUBLANES, pl.ds(n % SUBLANES, grid_rows, stride=SUBLANES), :]
        for k in range(upto):
            total = total + weight(n - k) * past[k, side, :]
        return total

    def beside(n):
        return past[n, pl.ds(SUBLANES - 1, grid_rows), :] + past[n, pl.ds(SUBLANES + 1, grid_rows), :]

    def keep(n, surface):
        past[n, side, :] = surface
        if n == 0:
            return
        g, t = (n - 1) // SUBLANES, (n - 1) % SUBLANES
        for j in range(cells // LANES):
            even = past[n, pl.ds(SUBLANES + 2 * j, tiles, stride=rows), :]
            odd = past[n, pl.ds(SUBLANES + 2 * j + 1, tiles, stride=rows), :]
            packed[j, g, pl.ds(t, tiles, stride=SUBLANES), :] = pick(lane, (face,), (even, pltpu.roll(odd, face, axis=1)))
        if t == SUBLANES - 1:
            now = pl.ds(g * SUBLANES, SUBLANES)
            for j in range(cells // LANES):
                for a in range(tiles):
                    tile = packed[j, g, pl.ds(a * SUBLANES, SUBLANES), :]
                    trace[a, now, pl.ds(j * LANES, LANES)] = tile.astype(jnp.bfloat16)
            if last:
                pltpu.make_async_copy(trace.at[:, now, :], away.at[:, now, :], done.at[g]).start()

    surface = fields[0]
    receive(0)
    keep(0, surface)
    stay = fields[1]
    for n in range(0, steps, 2):
        if n % SUBLANES == 0 and n // SUBLANES + 1 < groups:
            receive(n // SUBLANES + 1)
        still = (stay * surface + known(n, n)) + mix * beside(n)
        middle = still + mix * (west(surface) + east(surface))
        twice = (west(surface, 2) + east(surface, 2)) + (surface + surface)
        sides = (west(still) + east(still)) + mix * twice
        keep(n + 1, middle)
        surface = (stay * middle + known(n + 1, n + 1)) + mix * (beside(n + 1) + sides)
        keep(n + 2, surface)
    if last:
        for g in range(groups):
            now = pl.ds(g * SUBLANES, SUBLANES)
            pltpu.make_async_copy(trace.at[:, now, :], away.at[:, now, :], done.at[g]).wait()
    if first:
        fetch.wait()


def product(trace, halves, a):
    regrid, i = halves[a // halves[0].shape[0]], a % halves[0].shape[0]
    return lax.dot_general(trace[a], regrid[i], (((1,), (1,)), ((), ())), preferred_element_type=jnp.float32)


def redrive(trace, lower, upper, base, sea, chunk, drive):
    tiles, pairs, _, _ = base.shape
    for a in range(tiles):
        mapped = product(trace, (lower, upper), a)
        for j in range(pairs):
            slope = sea[a * pairs + j : a * pairs + j + 1, :]
            drive[a, j] = base[a, j] + slope * mapped[:, j * LANES : (j + 1) * LANES]
    ship(drive, chunk, LANES // 2)


def remap(trace, lower, upper, forcing, by_row):
    regrid = (lower, upper)
    tiles, steps, cells = trace.shape
    _, rows, width = forcing.shape
    face = cells // rows
    for k, cut in enumerate(tiles_of(width)):
        mapped = joined(product(trace, regrid, 2 * k), product(trace, regrid, 2 * k + 1), face)
        for p in range(rows):
            by_row[k, pl.ds(p, steps, stride=rows), :] = mapped[p]
        for t in range(steps):
            forcing[t, :, cut] = by_row[k, pl.ds(t * rows, rows), :]


def unforced(state, powers, rest, stack, levels, by_row):
    lev, rows, width = state.shape
    padded = powers.shape[1]
    steps = powers.shape[0] - 1
    fill = pl.ds(lev * rows, (padded - lev) * rows)
    row, lane = row_of(powers.shape[1:]), lane_of(powers.shape[1:])
    still = jnp.where(row == 0, 0.0, powers[steps])[:, :padded]
    for k, cut in enumerate(tiles_of(width)):
        for l in range(lev):
            levels[k, pl.ds(l * rows, rows), :] = state[l, :, cut]
        levels[k, fill, :] = jnp.zeros((fill.size, LANES), jnp.float32)
        for p in range(rows):
            own = levels[k, pl.ds(p, padded, stride=rows), :]
            end = jnp.dot(still, own, precision=EXACT, preferred_element_type=jnp.float32)
            by_row[k, pl.ds(p, padded, stride=rows), :] = end
        for l in range(lev):
            rest[l, :, cut] = by_row[k, pl.ds(l * rows, rows), :]
    left = jnp.zeros(row.shape, jnp.float32)
    for n in range(steps):
        left = jnp.where(lane == steps - 1 - n, powers[n][:, 0:1], left)
    for i in range(stack.shape[0]):
        part = left.astype(jnp.bfloat16)
        stack[i] = part
        left = left - part.astype(jnp.float32)


def finish(history, rest, stack, final_far, final, by_row, done):
    tiles, steps, cells = history.shape
    lev, rows, width = rest.shape
    padded = stack.shape[1]
    face = cells // rows
    for k, cut in enumerate(tiles_of(width)):
        seen = joined(history[2 * k].astype(jnp.float32), history[2 * k + 1].astype(jnp.float32), face)
        for p in range(rows):
            end = None
            for i in range(stack.shape[0]):
                part = jnp.dot(
                    stack[i][:, :steps], seen[p].astype(jnp.bfloat16), preferred_element_type=jnp.float32
                )
                end = part if end is None else end + part
            by_row[k, pl.ds(p, padded, stride=rows), :] = end
        for l in range(lev):
            final[k, l] = rest[l, :, cut] + by_row[k, pl.ds(l * rows, rows), :]
        pltpu.make_async_copy(final.at[k], final_far.at[:, :, cut], done.at[k]).start()
    for k, cut in enumerate(tiles_of(width)):
        pltpu.make_async_copy(final.at[k], final_far.at[:, :, cut], done.at[k]).wait()


def on_device(state, guess, regrid, regime, land, land_temp, exchange_rate, vertical, mixing):
    _, lev, rows, width = state.shape
    steps = guess.shape[1]
    tiles = lax.axis_size("tile")
    face = width // tiles
    cells = rows * face
    grid_rows = rows * tiles
    if 2 * face != LANES or LANES - face < 2 * steps or 2 * rows != SUBLANES or steps != 3 * SUBLANES:
        raise ValueError("unsupported sizes")
    padded = -(-lev // SUBLANES) * SUBLANES
    f32, bf16 = jnp.float32, jnp.bfloat16
    shape = jax.ShapeDtypeStruct
    state, guess, blocks = state[0], guess[0], regrid[0, 0]

    count = width // LANES
    by_row = shape((count, steps * rows, LANES), f32)
    levels = shape((count, padded * rows, LANES), f32)
    fields_shape = shape((2, grid_rows, LANES), f32)
    trace_shape = shape((tiles, steps, cells), bf16)
    groups = steps // SUBLANES
    sent = rows * steps * 3 // 4
    drive = shape((tiles, rows // 2, steps, LANES), f32)
    stepping = [
        shape((groups, grid_rows * SUBLANES, LANES), f32),
        shape((steps + 1, grid_rows + 2 * SUBLANES, LANES), f32),
        shape((cells // LANES, groups, tiles * SUBLANES, LANES), f32),
    ]

    arrays = (exchange_rate, vertical, mixing[None], regime[0], land[0], land_temp[0], state, guess, blocks)
    half = shape((tiles // 2,) + blocks.shape[1:], blocks.dtype)
    near = [pltpu.SMEM(a.shape, a.dtype) for a in arrays[:3]] + [shape(a.shape, a.dtype) for a in arrays[3:-1]]
    chunk, base, sea, memory, powers, lower = run(
        prepare,
        (
            shape((tiles, sent + 2 * rows, LANES), bf16),
            drive,
            shape((tiles * rows // 2, LANES), f32),
            shape((steps + SUBLANES, LANES), f32),
            shape((steps + 1, padded, LANES), f32),
            half,
        ),
        arrays,
        [by_row, shape((count, 4 * SUBLANES * rows, LANES), f32), drive] + near + [pltpu.SemaphoreType.DMA((len(arrays),))],
        far=len(arrays),
    )
    for sweep in range(ITERS):
        arrived = lax.all_to_all(chunk, "tile", split_axis=0, concat_axis=0, tiled=True)
        if sweep == 0:
            fields, trace, upper = run(
                functools.partial(evolve, True, False),
                (fields_shape, trace_shape, half),
                (blocks, memory, arrived),
                stepping + [pltpu.SemaphoreType.DMA(())],
                far=1,
            )
        else:
            trace, away = run(
                functools.partial(evolve, False, True),
                (trace_shape, trace_shape),
                (memory, arrived, fields),
                stepping + [pltpu.SemaphoreType.DMA((groups,))],
                outward=1,
            )
        partner = lax.ppermute(trace, "mp", [(0, 1), (1, 0)])
        if sweep < ITERS - 1:
            chunk = run(
                redrive,
                shape((tiles, sent, LANES), bf16),
                (partner, lower, upper, base, sea),
                [drive],
            )
    history = lax.all_to_all(away, "tile", split_axis=0, concat_axis=0, tiled=True)
    forcing = run(remap, shape((steps, rows, width), f32), (partner, lower, upper), [by_row])
    final_shape = shape((lev, rows, width), f32)
    rest, stack = run(unforced, (final_shape, shape((3, padded, LANES), bf16)), (state, powers), [levels, levels])
    final = run(
        finish,
        final_shape,
        (history, rest, stack),
        [shape((count, lev, rows, LANES), f32), levels, pltpu.SemaphoreType.DMA((count,))],
        outward=1,
    )
    return final[None], forcing[None]


def solution(mesh):
    return jax.shard_map(
        on_device,
        mesh=mesh,
        in_specs=(
            P("mp", None, "tile", None),
            P("mp", None, "tile", None),
            P("mp", "tile", None, None, None),
            P("mp", "tile", None),
            P("mp", "tile", None),
            P("mp", "tile", None),
            P("mp", None),
            P("mp", None),
            P("mp"),
        ),
        out_specs=(P("mp", None, "tile", None), P("mp", None, "tile", None)),
        check_vma=False,
    )
```

```python
import functools
import math

import jax
import jax.numpy as jnp
from jax import lax
from jax.experimental import pallas as pl
from jax.experimental.pallas import tpu as pltpu
from jax.sharding import PartitionSpec as P

ITERS = 2
LANES = 128
SUBLANES = 8
SPARE = 4 << 20
EXACT = lax.Precision.HIGHEST
VMEM = pl.BlockSpec(memory_space=pltpu.VMEM)
HBM = pl.BlockSpec(memory_space=pltpu.HBM)


def size_of(leaf):
    if len(leaf.shape) < 2:
        return 4096
    rows = -(-leaf.shape[-2] // SUBLANES) * SUBLANES
    lanes = -(-leaf.shape[-1] // LANES) * LANES
    return math.prod(leaf.shape[:-2]) * rows * lanes * 4


def run(kernel, out, arrays, scratch, far=0, outward=0, cost=1):
    leaves = jax.tree.leaves(out) + list(arrays[far:]) + [leaf for leaf in scratch if isinstance(leaf, jax.ShapeDtypeStruct)]
    return pl.pallas_call(
        kernel,
        out_shape=out,
        in_specs=[HBM] * far + [VMEM] * (len(arrays) - far),
        out_specs=(VMEM,) * (len(out) - outward) + (HBM,) * outward if isinstance(out, tuple) else (HBM if outward else VMEM),
        scratch_shapes=[leaf if not isinstance(leaf, jax.ShapeDtypeStruct) else pltpu.VMEM(leaf.shape, leaf.dtype) for leaf in scratch],
        compiler_params=pltpu.CompilerParams(vmem_limit_bytes=sum(map(size_of, leaves)) + SPARE),
        cost_estimate=pl.CostEstimate(flops=cost * 1000000, bytes_accessed=0, transcendentals=0),
        name=getattr(kernel, "__name__", "evolve"),
    )(*[a if a.size == 1 else pltpu.with_memory_space_constraint(a, pltpu.HBM) for a in arrays[:far]], *arrays[far:])


def lane_of(shape):
    return lax.broadcasted_iota(jnp.int32, shape, len(shape) - 1)


def row_of(shape):
    return lax.broadcasted_iota(jnp.int32, shape, 0)


def tiles_of(width):
    return [pl.ds(k * LANES, LANES) for k in range(width // LANES)]


def windows(tile, count, face):
    half = (LANES - face) // 2
    for k in range(count):
        own, left, right = tile(k), tile((k - 1) % count), tile((k + 1) % count)
        lane = lane_of(own.shape)
        yield 2 * k, jnp.where(lane < face + half, own, left)
        yield 2 * k + 1, pltpu.roll(jnp.where(lane < half, right, own), face, axis=1)


def exchanged(x, y, face):
    lane = lane_of(x.shape)
    return (
        jnp.where(lane < face, x, pltpu.roll(y, face, axis=1)),
        jnp.where(lane < face, pltpu.roll(x, face, axis=1), y),
    )


def joined(first, second, face):
    out = []
    for j in range(first.shape[1] // LANES):
        cut = slice(j * LANES, (j + 1) * LANES)
        out += exchanged(first[:, cut], second[:, cut], face)
    return out


def pick(lane, cuts, parts):
    out = parts[-1]
    for cut, part in zip(reversed(cuts), reversed(parts[:-1])):
        out = jnp.where(lane < cut, part, out)
    return out


def turn(x, by):
    return pltpu.roll(x, by % LANES, axis=1)


def ship(drive, chunk, face):
    tiles, pairs, _, _ = drive.shape
    lane = lane_of((SUBLANES, LANES)) % face
    for a in range(tiles):
        own, halo = {}, {}
        for j in range(pairs):
            for g in range(3):
                now = pl.ds(g * SUBLANES, SUBLANES)
                own[j, g] = drive[a, j, now, :]
                halo[j, g] = pick(lane, (face // 2,), (drive[(a + 1) % tiles, j, now, :], drive[(a - 1) % tiles, j, now, :]))
        out = [own[j, g] for j in range(pairs) for g in range(3)]
        for j in range(pairs):
            out.append(pick(lane, (24, 32, 40), (halo[j, 0], turn(halo[j, 2], 24), turn(halo[j, 2], -24), halo[j, 0])))
        out.append(pick(lane, (16, 32, 48), (halo[0, 1], turn(halo[1, 1], 16), turn(halo[1, 1], -16), halo[0, 1])))
        for i, tile in enumerate(out):
            chunk[a, pl.ds(i * SUBLANES, SUBLANES), :] = tile.astype(jnp.bfloat16)


def landed(arrived, a, face, g):
    lane = lane_of((SUBLANES, LANES))
    tile = lambda i: arrived[a, pl.ds(i * SUBLANES, SUBLANES), :].astype(jnp.float32)
    out = []
    for j in range(2):
        main = tile(3 * j + g)
        halo = tile(8) if g == 1 else tile(6 + j)
        if g == 0 or (g, j) == (1, 0):
            out.append(pick(lane, (face,), (main, turn(halo, face))))
            out.append(pick(lane, (face,), (turn(main, face), halo)))
        else:
            by = 16 if g == 1 else 24
            out.append(pick(lane, (face, 96), (main, turn(halo, face - by), turn(halo, face + by))))
            out.append(pick(lane, (face, 96), (turn(main, face), turn(halo, -by), turn(halo, by))))
    return out


def prepare(
    rates_far, vertical_far, mixing_far, regime_far, land_far, land_temp_far, state_far, guess_far, blocks_far,
    chunk, base, sea, memory, xs, blocks,
    by_row, levels, drive, rates, vertical, mixing, regime, land, land_temp, state, guess, done,
):
    pairs = (
        (rates_far, rates),
        (vertical_far, vertical),
        (mixing_far, mixing),
        (regime_far, regime),
        (land_far, land),
        (land_temp_far, land_temp),
        (state_far, state),
        (guess_far, guess),
        (blocks_far.at[pl.ds(0, blocks.shape[0])], blocks),
    )
    copies = [pltpu.make_async_copy(far, near, done.at[i]) for i, (far, near) in enumerate(pairs)]
    for copy in copies:
        copy.start()
    for copy in copies[:3]:
        copy.wait()
    lev, rows, width = state.shape
    steps = guess.shape[0]
    padded = xs.shape[1]
    deep = levels.shape[1] // rows
    face = width // chunk.shape[0]

    shape = (padded, LANES)
    row, lane = row_of(shape), lane_of(shape)
    up = jnp.zeros(shape, jnp.float32)
    down = jnp.zeros(shape, jnp.float32)
    for l in range(lev - 1):
        up = jnp.where((row == l) & (row > 0), vertical[0, l], up)
        down = jnp.where(row == l + 1, vertical[0, l], down)
    keep = jnp.where(row == 0, 0.0, 1.0 - up - down)
    power = jnp.where((row == lane) & (row < lev), 1.0, 0.0)
    first = jnp.zeros((steps, LANES), jnp.float32)
    for n in range(steps + 1):
        xs[n] = power
        if n == steps:
            break
        first = jnp.where(row_of(first.shape) == n, power[1:2, :], first)
        power = keep * power + up * pltpu.roll(power, padded - 1, axis=0) + down * pltpu.roll(power, 1, axis=0)
    v0 = vertical[0, 0]
    memory[pl.ds(0, steps), :] = jnp.broadcast_to(v0 * first[:, 0:1], first.shape)
    shape = (SUBLANES, LANES)
    row = row_of(shape)
    known = jnp.where(row == 0, 1.0 - v0 - 4.0 * mixing[0, 0], mixing[0, 0])
    for kind in range(rates.shape[1]):
        known = jnp.where(row == 2 + kind, rates[0, kind], known)
    memory[pl.ds(steps, SUBLANES), :] = known
    for copy in copies[3:-1]:
        copy.wait()
    own_cell = (lane_of(first.shape) == 0) & (row_of(first.shape) == 0)
    to_below = jnp.where(own_cell, 1.0 - v0 - 4.0 * mixing[0, 0], v0 * first)
    high = to_below.astype(jnp.bfloat16).astype(jnp.float32)
    low = to_below - high
    lane = lane_of(first.shape)
    to_below = pick(lane, (deep, 2 * deep), (high, pltpu.roll(high, deep, axis=1), pltpu.roll(low, 2 * deep, axis=1)))
    to_below = to_below[:, : 3 * deep].astype(jnp.bfloat16)

    coeff = jnp.zeros(regime.shape, jnp.float32)
    for kind in range(rates.shape[1]):
        coeff = jnp.where(regime[...] == kind, rates[0, kind], coeff)
    on_land = land[...] == 1
    open_sea = jnp.where(on_land, 0.0, coeff)
    fixed = jnp.where(on_land, coeff * land_temp[...], 0.0)
    left = state[0] - state[0].astype(jnp.bfloat16).astype(jnp.float32)
    taken = coeff * left

    count = width // LANES
    rest = pl.ds(lev * rows, (deep - lev) * rows)
    for k, cut in enumerate(tiles_of(width)):
        levels[k, pl.ds(0, rows), :] = left[:, k * LANES : (k + 1) * LANES]
        for l in range(1, lev):
            levels[k, pl.ds(l * rows, rows), :] = state[l, :, cut]
        levels[k, rest, :] = jnp.zeros((rest.size, LANES), jnp.float32)
        for t in range(steps):
            by_row[k, pl.ds(t * rows, rows), :] = guess[t, :, cut]
    def below(p, k):
        parts = []
        for i in (k, k + 1):
            own = levels[i, pl.ds(p, deep, stride=rows), :]
            near = own.astype(jnp.bfloat16)
            parts.append(jnp.concatenate([near, (own - near.astype(jnp.float32)).astype(jnp.bfloat16), near], axis=0))
        pair = jnp.dot(to_below, jnp.concatenate(parts, axis=1), preferred_element_type=jnp.float32)
        return pair[:, :LANES], pair[:, LANES:]

    for j in range(rows // 2):
        two = (2 * j, 2 * j + 1)
        for k in range(0, count, 2):
            for i, *parts in zip((k, k + 1), *[below(p, k) for p in two]):
                cut = slice(i * LANES, (i + 1) * LANES)
                start = row_of(parts[0].shape) == 0
                still = [part + jnp.where(start, fixed[p : p + 1, cut] - taken[p : p + 1, cut], fixed[p : p + 1, cut]) for p, part in zip(two, parts)]
                slopes = [open_sea[p : p + 1, cut] for p in two]
                forced = [
                    part + slope * by_row[i, pl.ds(p, steps, stride=rows), :] for p, part, slope in zip(two, still, slopes)
                ]
                for b, tile in enumerate(exchanged(*still, face)):
                    base[2 * i + b, j] = tile
                for b, tile in enumerate(exchanged(*forced, face)):
                    drive[2 * i + b, j] = tile
                for b, tile in enumerate(exchanged(*slopes, face)):
                    sea[pl.ds((2 * i + b) * (rows // 2) + j, 1), :] = tile
    ship(drive, chunk, face)
    fields = jnp.concatenate([state[0], regime[...].astype(jnp.float32)], axis=0)
    for a, window in windows(lambda k: fields[:, k * LANES : (k + 1) * LANES], count, face):
        chunk[a, pl.ds(chunk.shape[1] - 2 * rows, 2 * rows), :] = window.astype(jnp.bfloat16)
    copies[-1].wait()


def evolve(first, last, *refs):
    if first:
        blocks_far, memory, arrived, fields, trace, blocks, drive, past, packed, fetched = refs
        half = blocks.shape[0]
        fetch = pltpu.make_async_copy(blocks_far.at[pl.ds(half, half)], blocks, fetched)
        fetch.start()
    else:
        memory, arrived, fields, trace, away, drive, past, packed, done = refs
    tiles, steps, cells = trace.shape
    grid_rows = fields.shape[1]
    rows = grid_rows // tiles
    face = cells // rows
    groups = steps // SUBLANES
    side = pl.ds(SUBLANES, grid_rows)
    edge = jnp.zeros((SUBLANES, LANES), jnp.float32)

    @pl.loop(0, 5)
    def _(part):
        for n in range((steps + 1) // 5):
            past[part * ((steps + 1) // 5) + n, pl.ds(0, SUBLANES), :] = edge
            past[part * ((steps + 1) // 5) + n, pl.ds(SUBLANES + grid_rows, SUBLANES), :] = edge

    if first:
        for a in range(tiles):
            both = arrived[a, pl.ds(arrived.shape[1] - 2 * rows, 2 * rows), :].astype(jnp.float32)
            fields[0, pl.ds(a * rows, rows), :] = both[:rows]
            fields[1, pl.ds(a * rows, rows), :] = both[rows:]
        regime = fields[1]
        coeff = jnp.zeros(regime.shape, jnp.float32)
        for kind in range(memory.shape[0] - steps - 2):
            coeff = jnp.where(regime == kind, memory[steps + 2 + kind : steps + 3 + kind, :], coeff)
        fields[1] = memory[steps : steps + 1, :] - coeff
    mix = memory[steps + 1 : steps + 2, :]
    lane = lane_of((tiles, LANES))

    def west(x, by=1):
        return pltpu.roll(x, by, axis=1)

    def east(x, by=1):
        return pltpu.roll(x, LANES - by, axis=1)

    def weight(j):
        return memory[j : j + 1, :]

    def receive(g):
        for a in range(tiles):
            for p, tile in enumerate(landed(arrived, a, face, g)):
                drive[g, pl.ds((a * rows + p) * SUBLANES, SUBLANES), :] = tile

    def known(n, upto):
        total = drive[n // SUBLANES, pl.ds(n % SUBLANES, grid_rows, stride=SUBLANES), :]
        for k in range(upto):
            total = total + weight(n - k) * past[k, side, :]
        return total

    def beside(n):
        return past[n, pl.ds(SUBLANES - 1, grid_rows), :] + past[n, pl.ds(SUBLANES + 1, grid_rows), :]

    def keep(n, surface):
        past[n, side, :] = surface
        if n == 0:
            return
        g, t = (n - 1) // SUBLANES, (n - 1) % SUBLANES
        for j in range(cells // LANES):
            even = past[n, pl.ds(SUBLANES + 2 * j, tiles, stride=rows), :]
            odd = past[n, pl.ds(SUBLANES + 2 * j + 1, tiles, stride=rows), :]
            packed[j, g, pl.ds(t, tiles, stride=SUBLANES), :] = pick(lane, (face,), (even, pltpu.roll(odd, face, axis=1)))
        if t == SUBLANES - 1:
            now = pl.ds(g * SUBLANES, SUBLANES)
            for j in range(cells // LANES):
                for a in range(tiles):
                    tile = packed[j, g, pl.ds(a * SUBLANES, SUBLANES), :]
                    trace[a, now, pl.ds(j * LANES, LANES)] = tile.astype(jnp.bfloat16)
            if last:
                pltpu.make_async_copy(trace.at[:, now, :], away.at[:, now, :], done.at[g]).start()

    surface = fields[0]
    receive(0)
    keep(0, surface)
    stay = fields[1]
    for n in range(0, steps, 2):
        if n % SUBLANES == 0 and n // SUBLANES + 1 < groups:
            receive(n // SUBLANES + 1)
        still = (stay * surface + known(n, n)) + mix * beside(n)
        middle = still + mix * (west(surface) + east(surface))
        twice = (west(surface, 2) + east(surface, 2)) + (surface + surface)
        sides = (west(still) + east(still)) + mix * twice
        keep(n + 1, middle)
        surface = (stay * middle + known(n + 1, n + 1)) + mix * (beside(n + 1) + sides)
        keep(n + 2, surface)
    if last:
        for g in range(groups):
            now = pl.ds(g * SUBLANES, SUBLANES)
            pltpu.make_async_copy(trace.at[:, now, :], away.at[:, now, :], done.at[g]).wait()
    if first:
        fetch.wait()


def product(trace, halves, a):
    regrid, i = halves[a // halves[0].shape[0]], a % halves[0].shape[0]
    return lax.dot_general(trace[a], regrid[i], (((1,), (1,)), ((), ())), preferred_element_type=jnp.float32)


def redrive(trace, lower, upper, base, sea, chunk, drive):
    tiles, pairs, _, _ = base.shape
    for a in range(tiles):
        mapped = product(trace, (lower, upper), a)
        for j in range(pairs):
            slope = sea[a * pairs + j : a * pairs + j + 1, :]
            drive[a, j] = base[a, j] + slope * mapped[:, j * LANES : (j + 1) * LANES]
    ship(drive, chunk, LANES // 2)


def remap(trace, lower, upper, forcing, by_row):
    regrid = (lower, upper)
    tiles, steps, cells = trace.shape
    _, rows, width = forcing.shape
    face = cells // rows
    for k, cut in enumerate(tiles_of(width)):
        mapped = joined(product(trace, regrid, 2 * k), product(trace, regrid, 2 * k + 1), face)
        for p in range(rows):
            by_row[k, pl.ds(p, steps, stride=rows), :] = mapped[p]
        for t in range(steps):
            forcing[t, :, cut] = by_row[k, pl.ds(t * rows, rows), :]


def unforced(state, powers, rest, stack, levels, by_row):
    lev, rows, width = state.shape
    padded = powers.shape[1]
    steps = powers.shape[0] - 1
    fill = pl.ds(lev * rows, (padded - lev) * rows)
    row, lane = row_of(powers.shape[1:]), lane_of(powers.shape[1:])
    still = jnp.where(row == 0, 0.0, powers[steps])[:, :padded]
    for k, cut in enumerate(tiles_of(width)):
        for l in range(lev):
            levels[k, pl.ds(l * rows, rows), :] = state[l, :, cut]
        levels[k, fill, :] = jnp.zeros((fill.size, LANES), jnp.float32)
        for p in range(rows):
            own = levels[k, pl.ds(p, padded, stride=rows), :]
            end = jnp.dot(still, own, precision=EXACT, preferred_element_type=jnp.float32)
            by_row[k, pl.ds(p, padded, stride=rows), :] = end
        for l in range(lev):
            rest[l, :, cut] = by_row[k, pl.ds(l * rows, rows), :]
    left = jnp.zeros(row.shape, jnp.float32)
    for n in range(steps):
        left = jnp.where(lane == steps - 1 - n, powers[n][:, 0:1], left)
    for i in range(stack.shape[0]):
        part = left.astype(jnp.bfloat16)
        stack[i] = part
        left = left - part.astype(jnp.float32)


def finish(history, rest, stack, final_far, final, by_row, done):
    tiles, steps, cells = history.shape
    lev, rows, width = rest.shape
    padded = stack.shape[1]
    face = cells // rows
    for k, cut in enumerate(tiles_of(width)):
        seen = joined(history[2 * k].astype(jnp.float32), history[2 * k + 1].astype(jnp.float32), face)
        for p in range(rows):
            end = None
            for i in range(stack.shape[0]):
                part = jnp.dot(
                    stack[i][:, :steps], seen[p].astype(jnp.bfloat16), preferred_element_type=jnp.float32
                )
                end = part if end is None else end + part
            by_row[k, pl.ds(p, padded, stride=rows), :] = end
        for l in range(lev):
            final[k, l] = rest[l, :, cut] + by_row[k, pl.ds(l * rows, rows), :]
        pltpu.make_async_copy(final.at[k], final_far.at[:, :, cut], done.at[k]).start()
    for k, cut in enumerate(tiles_of(width)):
        pltpu.make_async_copy(final.at[k], final_far.at[:, :, cut], done.at[k]).wait()


def on_device(state, guess, regrid, regime, land, land_temp, exchange_rate, vertical, mixing):
    _, lev, rows, width = state.shape
    steps = guess.shape[1]
    tiles = lax.axis_size("tile")
    face = width // tiles
    cells = rows * face
    grid_rows = rows * tiles
    if 2 * face != LANES or LANES - face < 2 * steps or 2 * rows != SUBLANES or steps != 3 * SUBLANES:
        raise ValueError("unsupported sizes")
    padded = -(-lev // SUBLANES) * SUBLANES
    f32, bf16 = jnp.float32, jnp.bfloat16
    shape = jax.ShapeDtypeStruct
    state, guess, blocks = state[0], guess[0], regrid[0, 0]

    count = width // LANES
    by_row = shape((count, steps * rows, LANES), f32)
    levels = shape((count, padded * rows, LANES), f32)
    fields_shape = shape((2, grid_rows, LANES), f32)
    trace_shape = shape((tiles, steps, cells), bf16)
    groups = steps // SUBLANES
    sent = rows * steps * 3 // 4
    drive = shape((tiles, rows // 2, steps, LANES), f32)
    stepping = [
        shape((groups, grid_rows * SUBLANES, LANES), f32),
        shape((steps + 1, grid_rows + 2 * SUBLANES, LANES), f32),
        shape((cells // LANES, groups, tiles * SUBLANES, LANES), f32),
    ]

    arrays = (exchange_rate, vertical, mixing[None], regime[0], land[0], land_temp[0], state, guess, blocks)
    half = shape((tiles // 2,) + blocks.shape[1:], blocks.dtype)
    near = [pltpu.SMEM(a.shape, a.dtype) for a in arrays[:3]] + [shape(a.shape, a.dtype) for a in arrays[3:-1]]
    chunk, base, sea, memory, powers, lower = run(
        prepare,
        (
            shape((tiles, sent + 2 * rows, LANES), bf16),
            drive,
            shape((tiles * rows // 2, LANES), f32),
            shape((steps + SUBLANES, LANES), f32),
            shape((steps + 1, padded, LANES), f32),
            half,
        ),
        arrays,
        [by_row, shape((count, 4 * SUBLANES * rows, LANES), f32), drive] + near + [pltpu.SemaphoreType.DMA((len(arrays),))],
        far=len(arrays),
    )
    for sweep in range(ITERS):
        arrived = lax.all_to_all(chunk, "tile", split_axis=0, concat_axis=0, tiled=True)
        if sweep == 0:
            fields, trace, upper = run(
                functools.partial(evolve, True, False),
                (fields_shape, trace_shape, half),
                (blocks, memory, arrived),
                stepping + [pltpu.SemaphoreType.DMA(())],
                far=1,
            )
        else:
            trace, away = run(
                functools.partial(evolve, False, True),
                (trace_shape, trace_shape),
                (memory, arrived, fields),
                stepping + [pltpu.SemaphoreType.DMA((groups,))],
                outward=1,
            )
        partner = lax.ppermute(trace, "mp", [(0, 1), (1, 0)])
        if sweep < ITERS - 1:
            chunk = run(
                redrive,
                shape((tiles, sent, LANES), bf16),
                (partner, lower, upper, base, sea),
                [drive],
            )
    history = lax.all_to_all(away, "tile", split_axis=0, concat_axis=0, tiled=True)
    forcing = run(remap, shape((steps, rows, width), f32), (partner, lower, upper), [by_row])
    final_shape = shape((lev, rows, width), f32)
    rest, stack = run(unforced, (final_shape, shape((3, padded, LANES), bf16)), (state, powers), [levels, levels])
    final = run(
        finish,
        final_shape,
        (history, rest, stack),
        [shape((count, lev, rows, LANES), f32), levels, pltpu.SemaphoreType.DMA((count,))],
        outward=1,
    )
    return final[None], forcing[None]


def solution(mesh):
    return jax.shard_map(
        on_device,
        mesh=mesh,
        in_specs=(
            P("mp", None, "tile", None),
            P("mp", None, "tile", None),
            P("mp", "tile", None, None, None),
            P("mp", "tile", None),
            P("mp", "tile", None),
            P("mp", "tile", None),
            P("mp", None),
            P("mp", None),
            P("mp"),
        ),
        out_specs=(P("mp", None, "tile", None), P("mp", None, "tile", None)),
        check_vma=False,
    )
```

```python
import functools
import math

import jax
import jax.numpy as jnp
from jax import lax
from jax.experimental import pallas as pl
from jax.experimental.pallas import tpu as pltpu
from jax.sharding import PartitionSpec as P

ITERS = 2
LANES = 128
SUBLANES = 8
SPARE = 4 << 20
EXACT = lax.Precision.HIGHEST
VMEM = pl.BlockSpec(memory_space=pltpu.VMEM)
HBM = pl.BlockSpec(memory_space=pltpu.HBM)


def size_of(leaf):
    if len(leaf.shape) < 2:
        return 4096
    rows = -(-leaf.shape[-2] // SUBLANES) * SUBLANES
    lanes = -(-leaf.shape[-1] // LANES) * LANES
    return math.prod(leaf.shape[:-2]) * rows * lanes * 4


def run(kernel, out, arrays, scratch, far=0, outward=0, cost=1):
    leaves = jax.tree.leaves(out) + list(arrays[far:]) + [leaf for leaf in scratch if isinstance(leaf, jax.ShapeDtypeStruct)]
    return pl.pallas_call(
        kernel,
        out_shape=out,
        in_specs=[HBM] * far + [VMEM] * (len(arrays) - far),
        out_specs=(VMEM,) * (len(out) - outward) + (HBM,) * outward if isinstance(out, tuple) else (HBM if outward else VMEM),
        scratch_shapes=[leaf if not isinstance(leaf, jax.ShapeDtypeStruct) else pltpu.VMEM(leaf.shape, leaf.dtype) for leaf in scratch],
        compiler_params=pltpu.CompilerParams(vmem_limit_bytes=sum(map(size_of, leaves)) + SPARE),
        cost_estimate=pl.CostEstimate(flops=cost * 1000000, bytes_accessed=0, transcendentals=0),
        name=getattr(kernel, "__name__", "evolve"),
    )(*[a if a.size == 1 else pltpu.with_memory_space_constraint(a, pltpu.HBM) for a in arrays[:far]], *arrays[far:])


def lane_of(shape):
    return lax.broadcasted_iota(jnp.int32, shape, len(shape) - 1)


def row_of(shape):
    return lax.broadcasted_iota(jnp.int32, shape, 0)


def tiles_of(width):
    return [pl.ds(k * LANES, LANES) for k in range(width // LANES)]


def windows(tile, count, face):
    half = (LANES - face) // 2
    for k in range(count):
        own, left, right = tile(k), tile((k - 1) % count), tile((k + 1) % count)
        lane = lane_of(own.shape)
        yield 2 * k, jnp.where(lane < face + half, own, left)
        yield 2 * k + 1, pltpu.roll(jnp.where(lane < half, right, own), face, axis=1)


def exchanged(x, y, face):
    lane = lane_of(x.shape)
    return (
        jnp.where(lane < face, x, pltpu.roll(y, face, axis=1)),
        jnp.where(lane < face, pltpu.roll(x, face, axis=1), y),
    )


def joined(first, second, face):
    out = []
    for j in range(first.shape[1] // LANES):
        cut = slice(j * LANES, (j + 1) * LANES)
        out += exchanged(first[:, cut], second[:, cut], face)
    return out


def pick(lane, cuts, parts):
    out = parts[-1]
    for cut, part in zip(reversed(cuts), reversed(parts[:-1])):
        out = jnp.where(lane < cut, part, out)
    return out


def turn(x, by):
    return pltpu.roll(x, by % LANES, axis=1)


def ship(drive, chunk, face):
    tiles, pairs, _, _ = drive.shape
    lane = lane_of((SUBLANES, LANES)) % face
    for a in range(tiles):
        own, halo = {}, {}
        for j in range(pairs):
            for g in range(3):
                now = pl.ds(g * SUBLANES, SUBLANES)
                own[j, g] = drive[a, j, now, :]
                halo[j, g] = pick(lane, (face // 2,), (drive[(a + 1) % tiles, j, now, :], drive[(a - 1) % tiles, j, now, :]))
        out = [own[j, g] for j in range(pairs) for g in range(3)]
        for j in range(pairs):
            out.append(pick(lane, (24, 32, 40), (halo[j, 0], turn(halo[j, 2], 24), turn(halo[j, 2], -24), halo[j, 0])))
        out.append(pick(lane, (16, 32, 48), (halo[0, 1], turn(halo[1, 1], 16), turn(halo[1, 1], -16), halo[0, 1])))
        for i, tile in enumerate(out):
            chunk[a, pl.ds(i * SUBLANES, SUBLANES), :] = tile.astype(jnp.bfloat16)


def landed(arrived, a, face, g):
    lane = lane_of((SUBLANES, LANES))
    tile = lambda i: arrived[a, pl.ds(i * SUBLANES, SUBLANES), :].astype(jnp.float32)
    out = []
    for j in range(2):
        main = tile(3 * j + g)
        halo = tile(8) if g == 1 else tile(6 + j)
        if g == 0 or (g, j) == (1, 0):
            out.append(pick(lane, (face,), (main, turn(halo, face))))
            out.append(pick(lane, (face,), (turn(main, face), halo)))
        else:
            by = 16 if g == 1 else 24
            out.append(pick(lane, (face, 96), (main, turn(halo, face - by), turn(halo, face + by))))
            out.append(pick(lane, (face, 96), (turn(main, face), turn(halo, -by), turn(halo, by))))
    return out


def prepare(
    rates_far, vertical_far, mixing_far, regime_far, land_far, land_temp_far, state_far, guess_far, blocks_far,
    chunk, base, sea, memory, xs, blocks,
    by_row, levels, drive, rates, vertical, mixing, regime, land, land_temp, state, guess, done,
):
    pairs = (
        (rates_far, rates),
        (vertical_far, vertical),
        (mixing_far, mixing),
        (regime_far, regime),
        (land_far, land),
        (land_temp_far, land_temp),
        (state_far, state),
        (guess_far, guess),
        (blocks_far.at[pl.ds(0, blocks.shape[0])], blocks),
    )
    copies = [pltpu.make_async_copy(far, near, done.at[i]) for i, (far, near) in enumerate(pairs)]
    for copy in copies:
        copy.start()
    for copy in copies[:3]:
        copy.wait()
    lev, rows, width = state.shape
    steps = guess.shape[0]
    padded = xs.shape[1]
    deep = levels.shape[1] // rows
    face = width // chunk.shape[0]

    shape = (padded, LANES)
    row, lane = row_of(shape), lane_of(shape)
    up = jnp.zeros(shape, jnp.float32)
    down = jnp.zeros(shape, jnp.float32)
    for l in range(lev - 1):
        up = jnp.where((row == l) & (row > 0), vertical[0, l], up)
        down = jnp.where(row == l + 1, vertical[0, l], down)
    keep = jnp.where(row == 0, 0.0, 1.0 - up - down)
    power = jnp.where((row == lane) & (row < lev), 1.0, 0.0)
    first = jnp.zeros((steps, LANES), jnp.float32)
    for n in range(steps + 1):
        xs[n] = power
        if n == steps:
            break
        first = jnp.where(row_of(first.shape) == n, power[1:2, :], first)
        power = keep * power + up * pltpu.roll(power, padded - 1, axis=0) + down * pltpu.roll(power, 1, axis=0)
    v0 = vertical[0, 0]
    memory[pl.ds(0, steps), :] = jnp.broadcast_to(v0 * first[:, 0:1], first.shape)
    shape = (SUBLANES, LANES)
    row = row_of(shape)
    known = jnp.where(row == 0, 1.0 - v0 - 4.0 * mixing[0, 0], mixing[0, 0])
    for kind in range(rates.shape[1]):
        known = jnp.where(row == 2 + kind, rates[0, kind], known)
    memory[pl.ds(steps, SUBLANES), :] = known
    for copy in copies[3:-1]:
        copy.wait()
    own_cell = (lane_of(first.shape) == 0) & (row_of(first.shape) == 0)
    to_below = jnp.where(own_cell, 1.0 - v0 - 4.0 * mixing[0, 0], v0 * first)
    high = to_below.astype(jnp.bfloat16).astype(jnp.float32)
    low = to_below - high
    lane = lane_of(first.shape)
    to_below = pick(lane, (deep, 2 * deep), (high, pltpu.roll(high, deep, axis=1), pltpu.roll(low, 2 * deep, axis=1)))
    to_below = to_below[:, : 3 * deep].astype(jnp.bfloat16)

    coeff = jnp.zeros(regime.shape, jnp.float32)
    for kind in range(rates.shape[1]):
        coeff = jnp.where(regime[...] == kind, rates[0, kind], coeff)
    on_land = land[...] == 1
    open_sea = jnp.where(on_land, 0.0, coeff)
    fixed = jnp.where(on_land, coeff * land_temp[...], 0.0)
    left = state[0] - state[0].astype(jnp.bfloat16).astype(jnp.float32)
    taken = coeff * left

    count = width // LANES
    rest = pl.ds(lev * rows, (deep - lev) * rows)
    for k, cut in enumerate(tiles_of(width)):
        levels[k, pl.ds(0, rows), :] = left[:, k * LANES : (k + 1) * LANES]
        for l in range(1, lev):
            levels[k, pl.ds(l * rows, rows), :] = state[l, :, cut]
        levels[k, rest, :] = jnp.zeros((rest.size, LANES), jnp.float32)
        for t in range(steps):
            by_row[k, pl.ds(t * rows, rows), :] = guess[t, :, cut]
    def below(p, k):
        parts = []
        for i in (k, k + 1):
            own = levels[i, pl.ds(p, deep, stride=rows), :]
            near = own.astype(jnp.bfloat16)
            parts.append(jnp.concatenate([near, (own - near.astype(jnp.float32)).astype(jnp.bfloat16), near], axis=0))
        pair = jnp.dot(to_below, jnp.concatenate(parts, axis=1), preferred_element_type=jnp.float32)
        return pair[:, :LANES], pair[:, LANES:]

    for j in range(rows // 2):
        two = (2 * j, 2 * j + 1)
        for k in range(0, count, 2):
            for i, *parts in zip((k, k + 1), *[below(p, k) for p in two]):
                cut = slice(i * LANES, (i + 1) * LANES)
                start = row_of(parts[0].shape) == 0
                still = [part + jnp.where(start, fixed[p : p + 1, cut] - taken[p : p + 1, cut], fixed[p : p + 1, cut]) for p, part in zip(two, parts)]
                slopes = [open_sea[p : p + 1, cut] for p in two]
                forced = [
                    part + slope * by_row[i, pl.ds(p, steps, stride=rows), :] for p, part, slope in zip(two, still, slopes)
                ]
                for b, tile in enumerate(exchanged(*still, face)):
                    base[2 * i + b, j] = tile
                for b, tile in enumerate(exchanged(*forced, face)):
                    drive[2 * i + b, j] = tile
                for b, tile in enumerate(exchanged(*slopes, face)):
                    sea[pl.ds((2 * i + b) * (rows // 2) + j, 1), :] = tile
    ship(drive, chunk, face)
    fields = jnp.concatenate([state[0], regime[...].astype(jnp.float32)], axis=0)
    for a, window in windows(lambda k: fields[:, k * LANES : (k + 1) * LANES], count, face):
        chunk[a, pl.ds(chunk.shape[1] - 2 * rows, 2 * rows), :] = window.astype(jnp.bfloat16)
    copies[-1].wait()


def evolve(first, last, *refs):
    if first:
        blocks_far, memory, arrived, fields, trace, blocks, drive, past, packed, fetched = refs
        half = blocks.shape[0]
        fetch = pltpu.make_async_copy(blocks_far.at[pl.ds(half, half)], blocks, fetched)
        fetch.start()
    else:
        memory, arrived, fields, trace, away, drive, past, packed, done = refs
    tiles, steps, cells = trace.shape
    grid_rows = fields.shape[1]
    rows = grid_rows // tiles
    face = cells // rows
    groups = steps // SUBLANES
    side = pl.ds(SUBLANES, grid_rows)
    edge = jnp.zeros((SUBLANES, LANES), jnp.float32)

    @pl.loop(0, 5)
    def _(part):
        for n in range((steps + 1) // 5):
            past[part * ((steps + 1) // 5) + n, pl.ds(0, SUBLANES), :] = edge
            past[part * ((steps + 1) // 5) + n, pl.ds(SUBLANES + grid_rows, SUBLANES), :] = edge

    if first:
        for a in range(tiles):
            both = arrived[a, pl.ds(arrived.shape[1] - 2 * rows, 2 * rows), :].astype(jnp.float32)
            fields[0, pl.ds(a * rows, rows), :] = both[:rows]
            fields[1, pl.ds(a * rows, rows), :] = both[rows:]
        regime = fields[1]
        coeff = jnp.zeros(regime.shape, jnp.float32)
        for kind in range(memory.shape[0] - steps - 2):
            coeff = jnp.where(regime == kind, memory[steps + 2 + kind : steps + 3 + kind, :], coeff)
        fields[1] = memory[steps : steps + 1, :] - coeff
    mix = memory[steps + 1 : steps + 2, :]
    lane = lane_of((tiles, LANES))

    def west(x, by=1):
        return pltpu.roll(x, by, axis=1)

    def east(x, by=1):
        return pltpu.roll(x, LANES - by, axis=1)

    def weight(j):
        return memory[j : j + 1, :]

    def receive(g):
        for a in range(tiles):
            for p, tile in enumerate(landed(arrived, a, face, g)):
                drive[g, pl.ds((a * rows + p) * SUBLANES, SUBLANES), :] = tile

    def known(n, upto):
        total = drive[n // SUBLANES, pl.ds(n % SUBLANES, grid_rows, stride=SUBLANES), :]
        for k in range(upto):
            total = total + weight(n - k) * past[k, side, :]
        return total

    def beside(n):
        return past[n, pl.ds(SUBLANES - 1, grid_rows), :] + past[n, pl.ds(SUBLANES + 1, grid_rows), :]

    def keep(n, surface):
        past[n, side, :] = surface
        if n == 0:
            return
        g, t = (n - 1) // SUBLANES, (n - 1) % SUBLANES
        for j in range(cells // LANES):
            even = past[n, pl.ds(SUBLANES + 2 * j, tiles, stride=rows), :]
            odd = past[n, pl.ds(SUBLANES + 2 * j + 1, tiles, stride=rows), :]
            packed[j, g, pl.ds(t, tiles, stride=SUBLANES), :] = pick(lane, (face,), (even, pltpu.roll(odd, face, axis=1)))
        if t == SUBLANES - 1:
            now = pl.ds(g * SUBLANES, SUBLANES)
            for j in range(cells // LANES):
                for a in range(tiles):
                    tile = packed[j, g, pl.ds(a * SUBLANES, SUBLANES), :]
                    trace[a, now, pl.ds(j * LANES, LANES)] = tile.astype(jnp.bfloat16)
            if last:
                pltpu.make_async_copy(trace.at[:, now, :], away.at[:, now, :], done.at[g]).start()

    surface = fields[0]
    receive(0)
    keep(0, surface)
    stay = fields[1]
    for n in range(0, steps, 2):
        if n % SUBLANES == 0 and n // SUBLANES + 1 < groups:
            receive(n // SUBLANES + 1)
        still = (stay * surface + known(n, n)) + mix * beside(n)
        middle = still + mix * (west(surface) + east(surface))
        twice = (west(surface, 2) + east(surface, 2)) + (surface + surface)
        sides = (west(still) + east(still)) + mix * twice
        keep(n + 1, middle)
        surface = (stay * middle + known(n + 1, n + 1)) + mix * (beside(n + 1) + sides)
        keep(n + 2, surface)
    if last:
        for g in range(groups):
            now = pl.ds(g * SUBLANES, SUBLANES)
            pltpu.make_async_copy(trace.at[:, now, :], away.at[:, now, :], done.at[g]).wait()
    if first:
        fetch.wait()


def product(trace, halves, a):
    regrid, i = halves[a // halves[0].shape[0]], a % halves[0].shape[0]
    return lax.dot_general(trace[a], regrid[i], (((1,), (1,)), ((), ())), preferred_element_type=jnp.float32)


def redrive(trace, lower, upper, base, sea, chunk, drive):
    tiles, pairs, _, _ = base.shape
    for a in range(tiles):
        mapped = product(trace, (lower, upper), a)
        for j in range(pairs):
            slope = sea[a * pairs + j : a * pairs + j + 1, :]
            drive[a, j] = base[a, j] + slope * mapped[:, j * LANES : (j + 1) * LANES]
    ship(drive, chunk, LANES // 2)


def remap(trace, lower, upper, forcing, by_row):
    regrid = (lower, upper)
    tiles, steps, cells = trace.shape
    _, rows, width = forcing.shape
    face = cells // rows
    for k, cut in enumerate(tiles_of(width)):
        mapped = joined(product(trace, regrid, 2 * k), product(trace, regrid, 2 * k + 1), face)
        for p in range(rows):
            by_row[k, pl.ds(p, steps, stride=rows), :] = mapped[p]
        for t in range(steps):
            forcing[t, :, cut] = by_row[k, pl.ds(t * rows, rows), :]


def unforced(state, powers, rest, stack, levels, by_row):
    lev, rows, width = state.shape
    padded = powers.shape[1]
    steps = powers.shape[0] - 1
    fill = pl.ds(lev * rows, (padded - lev) * rows)
    row, lane = row_of(powers.shape[1:]), lane_of(powers.shape[1:])
    still = jnp.where(row == 0, 0.0, powers[steps])[:, :padded]
    for k, cut in enumerate(tiles_of(width)):
        for l in range(lev):
            levels[k, pl.ds(l * rows, rows), :] = state[l, :, cut]
        levels[k, fill, :] = jnp.zeros((fill.size, LANES), jnp.float32)
        for p in range(rows):
            own = levels[k, pl.ds(p, padded, stride=rows), :]
            end = jnp.dot(still, own, precision=EXACT, preferred_element_type=jnp.float32)
            by_row[k, pl.ds(p, padded, stride=rows), :] = end
        for l in range(lev):
            rest[l, :, cut] = by_row[k, pl.ds(l * rows, rows), :]
    left = jnp.zeros(row.shape, jnp.float32)
    for n in range(steps):
        left = jnp.where(lane == steps - 1 - n, powers[n][:, 0:1], left)
    for i in range(stack.shape[0] // padded):
        part = left.astype(jnp.bfloat16)
        stack[pl.ds(i * padded, padded), :] = part
        left = left - part.astype(jnp.float32)


def finish(history, rest, stack, final_far, final, by_row, done):
    tiles, steps, cells = history.shape
    lev, rows, width = rest.shape
    padded = by_row.shape[1] // rows
    face = cells // rows
    parts = stack[:, :steps]
    cuts = tiles_of(width)
    for k in range(0, len(cuts), 2):
        near = [
            joined(history[2 * i].astype(jnp.float32), history[2 * i + 1].astype(jnp.float32), face) for i in (k, k + 1)
        ]
        for p in range(rows):
            seen = jnp.concatenate([near[0][p], near[1][p]], axis=1).astype(jnp.bfloat16)
            ends = jnp.dot(parts, seen, preferred_element_type=jnp.float32)
            end = (ends[:padded] + ends[padded : 2 * padded]) + ends[2 * padded :]
            by_row[k, pl.ds(p, padded, stride=rows), :] = end[:, :LANES]
            by_row[k + 1, pl.ds(p, padded, stride=rows), :] = end[:, LANES:]
        for i in (k, k + 1):
            for l in range(lev):
                final[i, l] = rest[l, :, cuts[i]] + by_row[i, pl.ds(l * rows, rows), :]
            pltpu.make_async_copy(final.at[i], final_far.at[:, :, cuts[i]], done.at[i]).start()
    for k, cut in enumerate(tiles_of(width)):
        pltpu.make_async_copy(final.at[k], final_far.at[:, :, cut], done.at[k]).wait()


def on_device(state, guess, regrid, regime, land, land_temp, exchange_rate, vertical, mixing):
    _, lev, rows, width = state.shape
    steps = guess.shape[1]
    tiles = lax.axis_size("tile")
    face = width // tiles
    cells = rows * face
    grid_rows = rows * tiles
    if 2 * face != LANES or LANES - face < 2 * steps or 2 * rows != SUBLANES or steps != 3 * SUBLANES:
        raise ValueError("unsupported sizes")
    padded = -(-lev // SUBLANES) * SUBLANES
    f32, bf16 = jnp.float32, jnp.bfloat16
    shape = jax.ShapeDtypeStruct
    state, guess, blocks = state[0], guess[0], regrid[0, 0]

    count = width // LANES
    by_row = shape((count, steps * rows, LANES), f32)
    levels = shape((count, padded * rows, LANES), f32)
    fields_shape = shape((2, grid_rows, LANES), f32)
    trace_shape = shape((tiles, steps, cells), bf16)
    groups = steps // SUBLANES
    sent = rows * steps * 3 // 4
    drive = shape((tiles, rows // 2, steps, LANES), f32)
    stepping = [
        shape((groups, grid_rows * SUBLANES, LANES), f32),
        shape((steps + 1, grid_rows + 2 * SUBLANES, LANES), f32),
        shape((cells // LANES, groups, tiles * SUBLANES, LANES), f32),
    ]

    arrays = (exchange_rate, vertical, mixing[None], regime[0], land[0], land_temp[0], state, guess, blocks)
    half = shape((tiles // 2,) + blocks.shape[1:], blocks.dtype)
    near = [pltpu.SMEM(a.shape, a.dtype) for a in arrays[:3]] + [shape(a.shape, a.dtype) for a in arrays[3:-1]]
    chunk, base, sea, memory, powers, lower = run(
        prepare,
        (
            shape((tiles, sent + 2 * rows, LANES), bf16),
            drive,
            shape((tiles * rows // 2, LANES), f32),
            shape((steps + SUBLANES, LANES), f32),
            shape((steps + 1, padded, LANES), f32),
            half,
        ),
        arrays,
        [by_row, shape((count, 4 * SUBLANES * rows, LANES), f32), drive] + near + [pltpu.SemaphoreType.DMA((len(arrays),))],
        far=len(arrays),
    )
    for sweep in range(ITERS):
        arrived = lax.all_to_all(chunk, "tile", split_axis=0, concat_axis=0, tiled=True)
        if sweep == 0:
            fields, trace, upper = run(
                functools.partial(evolve, True, False),
                (fields_shape, trace_shape, half),
                (blocks, memory, arrived),
                stepping + [pltpu.SemaphoreType.DMA(())],
                far=1,
            )
        else:
            trace, away = run(
                functools.partial(evolve, False, True),
                (trace_shape, trace_shape),
                (memory, arrived, fields),
                stepping + [pltpu.SemaphoreType.DMA((groups,))],
                outward=1,
            )
        partner = lax.ppermute(trace, "mp", [(0, 1), (1, 0)])
        if sweep < ITERS - 1:
            chunk = run(
                redrive,
                shape((tiles, sent, LANES), bf16),
                (partner, lower, upper, base, sea),
                [drive],
            )
    history = lax.all_to_all(away, "tile", split_axis=0, concat_axis=0, tiled=True)
    forcing = run(remap, shape((steps, rows, width), f32), (partner, lower, upper), [by_row])
    final_shape = shape((lev, rows, width), f32)
    rest, stack = run(unforced, (final_shape, shape((3 * padded, LANES), bf16)), (state, powers), [levels, levels])
    final = run(
        finish,
        final_shape,
        (history, rest, stack),
        [shape((count, lev, rows, LANES), f32), levels, pltpu.SemaphoreType.DMA((count,))],
        outward=1,
    )
    return final[None], forcing[None]


def solution(mesh):
    return jax.shard_map(
        on_device,
        mesh=mesh,
        in_specs=(
            P("mp", None, "tile", None),
            P("mp", None, "tile", None),
            P("mp", "tile", None, None, None),
            P("mp", "tile", None),
            P("mp", "tile", None),
            P("mp", "tile", None),
            P("mp", None),
            P("mp", None),
            P("mp"),
        ),
        out_specs=(P("mp", None, "tile", None), P("mp", None, "tile", None)),
        check_vma=False,
    )
```
